128 devices in a mesh: fsdp: 128 (over z, y, x, core).
Axes of the slice: x: 4, y: 4, z: 4, core: 2. Of those that a mesh axis runs over, the one named last changes fastest.
Arguments:
- x: bfloat16 [2, 131072, 960], P(None, 'fsdp')
- g: bfloat16 [2, 131072, 960], P(None, 'fsdp')
- w_gate: bfloat16 [1, 2457600], P(None, 'fsdp')
- w_up: bfloat16 [1, 2457600], P(None, 'fsdp')
- w_down: bfloat16 [1, 2457600], P(None, 'fsdp')
Outputs:
- output 1: bfloat16 [2, 131072, 960], P(None, 'fsdp')
- output 2: float32 [1, 2457600], P(None, 'fsdp')
- output 3: float32 [1, 2457600], P(None, 'fsdp')
- output 4: float32 [1, 2457600], P(None, 'fsdp')
All inputs are finite; a program needn't handle non-finite values.
Results may differ from the reference program's by a relative error of at most 0.001.
Values are sent between devices in bfloat16 or wider.
A program may use at most 1 GiB of HBM per device.

```python
import jax
import jax.numpy as jnp
from jax import lax

D = 960
FF = 2560
LAYERS = 1
MICRO = 2
TOK = 1024
GROUP = 128


def gelu_tanh(z):
    return jax.nn.gelu(z, approximate=True)


def setup_inputs(seed: int = 0) -> dict:
    key_list = jax.random.split(jax.random.key(seed), 5)
    rows = GROUP * TOK
    cot_scale = (MICRO * rows) ** -0.5
    down_scale = 0.5 * (FF * LAYERS) ** -0.5
    x = jax.random.normal(key_list[0], (MICRO, rows, D), jnp.float32)
    g = jax.random.normal(key_list[1], (MICRO, rows, D), jnp.float32) * cot_scale
    w_gate = jax.random.normal(key_list[2], (LAYERS, D * FF), jnp.float32) * D ** -0.5
    w_up = jax.random.normal(key_list[3], (LAYERS, D * FF), jnp.float32) * D ** -0.5
    w_down = jax.random.normal(key_list[4], (LAYERS, FF * D), jnp.float32) * down_scale
    return {"x": x.astype(jnp.bfloat16), "g": g.astype(jnp.bfloat16), "w_gate": w_gate.astype(jnp.bfloat16), "w_up": w_up.astype(jnp.bfloat16), "w_down": w_down.astype(jnp.bfloat16)}


def layer_forward(x_in, gate_w, up_w, down_w):
    pre_gate = jnp.dot(x_in, gate_w, preferred_element_type=jnp.float32).astype(jnp.bfloat16)
    pre_up = jnp.dot(x_in, up_w, preferred_element_type=jnp.float32).astype(jnp.bfloat16)
    hidden = (gelu_tanh(pre_gate.astype(jnp.float32)) * pre_up.astype(jnp.float32)).astype(jnp.bfloat16)
    mixed = x_in.astype(jnp.float32) + jnp.dot(hidden, down_w, preferred_element_type=jnp.float32)
    return mixed.astype(jnp.bfloat16), pre_gate, pre_up


def layer_backward(d_out, x_in, pre_gate, pre_up, gate_w, up_w, down_w):
    up_float = pre_up.astype(jnp.float32)
    gelu_val, gelu_vjp = jax.vjp(gelu_tanh, pre_gate.astype(jnp.float32))
    hidden = (gelu_val * up_float).astype(jnp.bfloat16)
    d_hidden = jnp.dot(d_out, down_w.T, preferred_element_type=jnp.float32).astype(jnp.bfloat16).astype(jnp.float32)
    d_gate = gelu_vjp(d_hidden * up_float)[0].astype(jnp.bfloat16)
    d_up = (d_hidden * gelu_val).astype(jnp.bfloat16)
    back_sum = jnp.dot(d_gate, gate_w.T, preferred_element_type=jnp.float32) + jnp.dot(d_up, up_w.T, preferred_element_type=jnp.float32)
    d_in = (d_out.astype(jnp.float32) + back_sum).astype(jnp.bfloat16)
    grad_g = jnp.dot(x_in.T, d_gate, preferred_element_type=jnp.float32)
    grad_u = jnp.dot(x_in.T, d_up, preferred_element_type=jnp.float32)
    grad_d = jnp.dot(hidden.T, d_out, preferred_element_type=jnp.float32)
    return d_in, grad_g, grad_u, grad_d


def reference(x, g, w_gate, w_up, w_down):
    gates = w_gate.reshape(LAYERS, D, FF)
    ups = w_up.reshape(LAYERS, D, FF)
    downs = w_down.reshape(LAYERS, FF, D)
    x_blocks = x.reshape(MICRO * GROUP, TOK, D)
    g_blocks = g.reshape(MICRO * GROUP, TOK, D)

    def block_step(running, block):
        x_in, cotangent = block

        def fwd_step(current, weights):
            out, pre_gate, pre_up = layer_forward(current, weights[0], weights[1], weights[2])
            return out, (current, pre_gate, pre_up)

        y_out, saved = lax.scan(fwd_step, x_in, (gates, ups, downs))

        def bwd_step(d_current, item):
            d_in, grad_g, grad_u, grad_d = layer_backward(d_current, item[0], item[1], item[2], item[3], item[4], item[5])
            return d_in, (grad_g, grad_u, grad_d)

        grads = lax.scan(bwd_step, cotangent, (saved[0], saved[1], saved[2], gates, ups, downs), reverse=True)[1]
        running = (running[0] + grads[0], running[1] + grads[1], running[2] + grads[2])
        return running, y_out

    zeros_in = jnp.zeros((LAYERS, D, FF), jnp.float32)
    zeros_out = jnp.zeros((LAYERS, FF, D), jnp.float32)
    running, y_blocks = lax.scan(block_step, (zeros_in, zeros_in, zeros_out), (x_blocks, g_blocks))
    y = y_blocks.reshape(MICRO, GROUP * TOK, D)
    return (y, running[0].reshape(LAYERS, D * FF), running[1].reshape(LAYERS, D * FF), running[2].reshape(LAYERS, FF * D))
```

```python
import jax
import jax.numpy as jnp
from jax import lax
from jax.experimental import pallas as pl
from jax.experimental.pallas import tpu as pltpu
from jax.sharding import PartitionSpec as P

AX = "fsdp"
MESH = pl.DeviceIdType.MESH
N = 4
WIDTH = 960
HID = 2560
HALF = 1280
ROWS = 1024
PAD = 1024
WAVES = (10, 10, 8)
PER_MICRO = (5, 5, 4)
CHUNK = ((16, 256), (16, 256), (40, 128))
SPLIT = (8, 8, 24)
REDUCE_DIMS = ((0, 1, 2), (1, 2, 0), (2, 0, 1))
GATHER_DIMS = ((2, 1, 0), (1, 0, 2), (0, 2, 1))


def place():
    me = lax.axis_index(AX)
    return (me // 32, (me // 8) % 4, (me // 2) % 4), me % 2


def device(pos, core):
    return (((pos[0] * 4 + pos[1]) * 4 + pos[2]) * 2 + core,)


def shifted(pos, dim, by):
    moved = list(pos)
    moved[dim] = (pos[dim] + by + N) % N
    return tuple(moved)


def greet(pos, core):
    barrier = pltpu.get_barrier_semaphore()
    others = [device(shifted(pos, dim, by), core) for dim in range(3) for by in (1, -1)] + [device(pos, 1 - core)]
    for other in others:
        pl.semaphore_signal(barrier, inc=1, device_id=other, device_id_type=MESH)
    pl.semaphore_wait(barrier, len(others))


def gather_kernel(x_own, g_own, w_gate, w_up, w_down, x_sib, g_sib, o_gate, o_up, o_down, send_sem, recv_sem, pair_sem):
    pos, core = place()
    greet(pos, core)
    pair = []
    for i, (src, dst) in enumerate(((x_own, x_sib), (g_own, g_sib))):
        pair.append(pltpu.make_async_remote_copy(src_ref=src, dst_ref=dst, send_sem=pair_sem.at[2 * i], recv_sem=pair_sem.at[2 * i + 1], device_id=device(pos, 1 - core), device_id_type=MESH))
        pair[i].start()
    pieces = (w_gate, w_up, w_down)
    outs = (o_gate, o_up, o_down)
    for s in range(3):
        outs[s][pos[0], pos[1], pos[2]] = pieces[s][...]

    def block(s, phase, by):
        dims = GATHER_DIMS[s]
        index = list(shifted(pos, dims[phase], by))
        for dim in dims[:phase]:
            index[dim] = slice(None)
        return tuple(index)

    def copy(s, phase, kind, src, dst):
        to = device(shifted(pos, GATHER_DIMS[s][phase], 1 if kind % 2 == 0 else -1), core)
        return pltpu.make_async_remote_copy(src_ref=src, dst_ref=dst, send_sem=send_sem.at[s, phase, kind], recv_sem=recv_sem.at[s, phase, kind], device_id=to, device_id_type=MESH)

    copies = []
    for phase in range(3):
        first = []
        for s in range(3):
            mine = outs[s].at[block(s, phase, 0)]
            src = pieces[s] if phase == 0 else mine
            first.append([copy(s, phase, kind, src, mine) for kind in range(2)])
            for c in first[s]:
                c.start()
        second = []
        for s in range(3):
            lanes = outs[s].shape[-1] // 2
            row = []
            for kind in range(2):
                first[s][kind].wait_recv()
                part = outs[s].at[block(s, phase, -1 if kind == 0 else 1)]
                part = part.at[(slice(None),) * (len(part.shape) - 1) + (pl.ds(kind * lanes, lanes),)]
                row.append(copy(s, phase, 2 + kind, part, part))
                row[kind].start()
            second.append(row)
        for s in range(3):
            for c in second[s]:
                c.wait_recv()
            copies += first[s] + second[s]
    for c in copies:
        c.wait_send()
    for c in pair:
        c.wait()


def gather(x_own, g_own, w_gate, w_up, w_down):
    shapes = [w.shape for w in (w_gate, w_up, w_down)]
    vmem = pl.BlockSpec(memory_space=pltpu.VMEM)
    hbm = pl.BlockSpec(memory_space=pl.ANY)
    return pl.pallas_call(
        gather_kernel,
        out_shape=[jax.ShapeDtypeStruct(x_own.shape, x_own.dtype), jax.ShapeDtypeStruct(g_own.shape, g_own.dtype)] + [jax.ShapeDtypeStruct((N, N, N) + s, jnp.bfloat16) for s in shapes],
        in_specs=[hbm, hbm, vmem, vmem, vmem],
        out_specs=[hbm, hbm, vmem, vmem, vmem],
        scratch_shapes=[pltpu.SemaphoreType.DMA((3, 3, 4)), pltpu.SemaphoreType.DMA((3, 3, 4)), pltpu.SemaphoreType.DMA((4,))],
        compiler_params=pltpu.CompilerParams(collective_id=0, has_side_effects=True, vmem_limit_bytes=40 * 2**20),
        name="gather_weights",
    )(x_own, g_own, w_gate, w_up, w_down)


def reduce_kernel(x_o, x_s, da_o, da_s, du_o, du_s, h_o, h_s, g_o, g_s, out_g, out_u, out_d, *scratch):
    (xv, hv, dav, duv, gv) = scratch[:5]
    part = scratch[5:8]
    line = scratch[8:11]
    point = scratch[11:14]
    inbox = [scratch[14 + 6 * s : 20 + 6 * s] for s in range(3)]
    send_sem, recv_sem, keep_sem, load_sem = scratch[32:]
    outs = (out_g, out_u, out_d)
    pos, core = place()

    def keep(kind, micro):
        hbm, vmem = ((x_o, x_s), xv) if kind == 0 else ((h_o, h_s), hv)
        return [pltpu.make_async_copy(hbm[i].at[pl.ds(micro * ROWS, ROWS)], vmem.at[micro, pl.ds(i * ROWS, ROWS)], keep_sem.at[kind, micro, i]) for i in range(2)]

    def load(s, wave):
        micro, q = wave // PER_MICRO[s], wave % PER_MICRO[s]
        hbm, vmem = (((da_o, da_s), dav), ((du_o, du_s), duv), ((g_o, g_s), gv))[s]
        lanes = pl.ds(pl.multiple_of(q * 256, 256), 256)
        rows = pl.ds(pl.multiple_of(micro * ROWS, ROWS), ROWS)
        return [pltpu.make_async_copy(hbm[i].at[rows, lanes], vmem.at[wave % 2, pl.ds(i * ROWS, ROWS)], load_sem.at[s, wave % 2, i]) for i in range(2)]

    for micro in range(2):
        for kind in range(2):
            for c in keep(kind, micro):
                c.start()
        if micro == 0:
            for s in range(3):
                for c in load(s, 0):
                    c.start()
    greet(pos, core)

    def send(s, kind, way, wave):
        dims = REDUCE_DIMS[s]
        phase, step = kind // 2, kind % 2
        dim = dims[phase]
        rest = [d for d in range(3) if d not in dims[:phase]]
        buf = (part, line, point)[phase][s].at[wave % 3]
        dest = (pos[dim] + (2 if step == 0 else (1 if way == 0 else 3))) % N
        index = [slice(None)] * len(rest)
        index[rest.index(dim)] = dest
        src = buf.at[tuple(index)]
        dst = inbox[s][kind].at[wave % 4, way]
        if step == 0:
            src = src.at[half(s, phase, way)]
            if phase == 2:
                dst = dst.at[pl.ds(0, half_rows(s, way))]
        to = device(shifted(pos, dim, 1 if way == 0 else -1), core)
        return pltpu.make_async_remote_copy(src_ref=src, dst_ref=dst, send_sem=send_sem.at[s, kind, way, wave % 4], recv_sem=recv_sem.at[s, kind, way, wave % 4], device_id=to, device_id_type=MESH)

    def half_rows(s, way):
        return CHUNK[s][0] - SPLIT[s] if way == 0 else SPLIT[s]

    def half(s, phase, way):
        if phase == 2:
            return pl.ds(SPLIT[s], CHUNK[s][0] - SPLIT[s]) if way == 0 else pl.ds(0, SPLIT[s])
        return pl.ds(2, 2) if way == 0 else pl.ds(0, 2)

    def make(s, wave):
        micro, q = wave // PER_MICRO[s], wave % PER_MICRO[s]
        for c in load(s, wave):
            c.wait()
        lhs, rhs = ((xv, dav), (xv, duv), (hv, gv))[s]
        tile = 512 if s < 2 else 640
        for i in range(2):
            r = lax.dot_general(lhs[micro, :, i * tile : (i + 1) * tile], rhs[wave % 2], (((0,), (0,)), ((), ())), preferred_element_type=jnp.float32)
            if s < 2:
                part[s][wave % 3, 2 * i : 2 * i + 2] = r.reshape(2, N, N, 16, 256)
            else:
                r = r.reshape(2, N, 2, 40, 256)
                for m in range(2):
                    for j in range(2):
                        part[s][wave % 3, 2 * i : 2 * i + 2, :, 2 * m + j] = r[:, :, m, :, 128 * j : 128 * j + 128]

    def stage(s, step, wave):
        if step > 0:
            kind = step - 1
            phase = kind // 2
            dims = REDUCE_DIMS[s]
            dim = dims[phase]
            rest = [d for d in range(3) if d not in dims[:phase]]
            at = rest.index(dim)
            buf = (part, line, point)[phase][s]
            arrived = inbox[s][kind]
            for way in range(2):
                send(s, kind, way, wave).wait_recv()
            if kind % 2 == 0:
                for way in range(2):
                    index = [slice(None)] * len(rest)
                    index[at] = (pos[dim] + (1 if way == 0 else 3)) % N
                    index = [wave % 3] + index
                    if phase == 2:
                        index.append(half(s, phase, way))
                        buf[tuple(index)] += arrived[wave % 4, way, : half_rows(s, way)]
                    else:
                        first = [i for i in range(1, len(index)) if i != at + 1][0]
                        index[first] = half(s, phase, way)
                        buf[tuple(index)] += arrived[wave % 4, way]
            else:
                index = [slice(None)] * len(rest)
                index[at] = pos[dim]
                total = buf[tuple([wave % 3] + index)] + arrived[wave % 4, 0] + arrived[wave % 4, 1]
                for way in range(2):
                    send(s, kind - 1, way, wave).wait_send()
                    send(s, kind, way, wave).wait_send()
                if phase < 2:
                    (line, point)[phase][s][wave % 3] = total
                else:
                    micro, q = wave // PER_MICRO[s], wave % PER_MICRO[s]
                    lanes = pl.ds(pl.multiple_of(q * CHUNK[s][1], CHUNK[s][1]), CHUNK[s][1])

                    @pl.when(micro == 0)
                    def _():
                        outs[s][:, lanes] = total

                    @pl.when(micro == 1)
                    def _():
                        outs[s][:, lanes] += total
        if step < 6:
            for way in range(2):
                send(s, step, way, wave).start()

    @pl.loop(0, 16)
    def _(slot):
        for kind, when in ((0, 5), (1, 4)):
            for micro in range(2):

                @pl.when(slot == micro * when)
                def _():
                    for c in keep(kind, micro):
                        c.wait()

        for s in range(3):

            @pl.when(slot + 1 < WAVES[s])
            def _():
                for c in load(s, slot + 1):
                    c.start()

        for s in range(3):

            @pl.when(slot < WAVES[s])
            def _():
                make(s, slot)
                stage(s, 0, slot)

        for step in range(1, 7):
            for s in range(3):

                @pl.when((slot >= step) & (slot - step < WAVES[s]))
                def _():
                    stage(s, step, slot - step)


def reduce_gradients(*operands):
    hbm = pl.BlockSpec(memory_space=pl.ANY)
    vmem = pl.BlockSpec(memory_space=pltpu.VMEM)
    f32 = jnp.float32
    bf16 = jnp.bfloat16
    scratch = [pltpu.VMEM((2, 2 * ROWS, PAD), bf16), pltpu.VMEM((2, 2 * ROWS, HALF), bf16)]
    scratch += [pltpu.VMEM((2, 2 * ROWS, 256), bf16) for s in range(3)]
    scratch += [pltpu.VMEM((3, N, N, N) + CHUNK[s], f32) for s in range(3)]
    scratch += [pltpu.VMEM((3, N, N) + CHUNK[s], f32) for s in range(3)]
    scratch += [pltpu.VMEM((3, N) + CHUNK[s], f32) for s in range(3)]
    for s in range(3):
        scratch += [pltpu.VMEM((4, 2) + lead + CHUNK[s], f32) for lead in ((2, N), (N, N), (2,), (N,))]
        scratch += [pltpu.VMEM((4, 2, SPLIT[s], CHUNK[s][1]), f32), pltpu.VMEM((4, 2) + CHUNK[s], f32)]
    scratch += [pltpu.SemaphoreType.DMA((3, 6, 2, 4)), pltpu.SemaphoreType.DMA((3, 6, 2, 4)), pltpu.SemaphoreType.DMA((2, 2, 2)), pltpu.SemaphoreType.DMA((3, 2, 2))]
    return pl.pallas_call(
        reduce_kernel,
        out_shape=[jax.ShapeDtypeStruct((16, HALF), f32), jax.ShapeDtypeStruct((16, HALF), f32), jax.ShapeDtypeStruct((40, 512), f32)],
        in_specs=[hbm] * 10,
        out_specs=[vmem] * 3,
        scratch_shapes=scratch,
        compiler_params=pltpu.CompilerParams(collective_id=1, has_side_effects=True, vmem_limit_bytes=62 * 2**20),
        name="reduce_gradients",
    )(*operands)


def gelu_tanh(z):
    return jax.nn.gelu(z, approximate=True)


def dot(a, b, dims=((1,), (0,))):
    return lax.dot_general(a, b, (dims, ((), ())), preferred_element_type=jnp.float32)


def activations(x_in, d_out, gate_w, up_w, down_w):
    pre_gate = dot(x_in, gate_w).astype(jnp.bfloat16)
    pre_up = dot(x_in, up_w).astype(jnp.bfloat16)
    up_float = pre_up.astype(jnp.float32)
    gelu_val, gelu_vjp = jax.vjp(gelu_tanh, pre_gate.astype(jnp.float32))
    hidden = (gelu_val * up_float).astype(jnp.bfloat16)
    d_hidden = dot(d_out, down_w, ((1,), (1,))).astype(jnp.bfloat16).astype(jnp.float32)
    d_gate = gelu_vjp(d_hidden * up_float)[0].astype(jnp.bfloat16)
    d_up = (d_hidden * gelu_val).astype(jnp.bfloat16)
    return hidden, d_gate, d_up


def solution(mesh):
    row_spec = P(None, AX, None)
    flat_spec = P(None, AX)
    sibling = [(i, i ^ 1) for i in range(128)]

    def spread():
        row = lax.broadcasted_iota(jnp.int32, (WIDTH, PAD), 0)
        col = lax.broadcasted_iota(jnp.int32, (WIDTH, PAD), 1)
        x_pad = (col == (row // 15) * 16 + row % 15).astype(jnp.bfloat16)
        e = row % 480
        g_pad = (col == (e // 128) * 256 + (row // 480) * 128 + e % 128).astype(jnp.bfloat16)
        return x_pad, g_pad

    def device_step(x, g, w_gate, w_up, w_down):
        core = lax.axis_index(AX) % 2
        odd = (lax.axis_index(AX) // 2) % 2
        x_pad, g_pad = spread()
        x_flat = x.reshape(2 * ROWS, WIDTH)
        g_flat = g.reshape(2 * ROWS, WIDTH)
        x_own = dot(x_flat, x_pad).astype(jnp.bfloat16)
        g_own = dot(g_flat, g_pad).astype(jnp.bfloat16)

        both = jnp.concatenate([w_gate, w_up], axis=0)
        other = lax.ppermute(both, AX, sibling)
        low = jnp.where(core == 0, both, other)
        high = jnp.where(core == 0, other, both)
        chip = jnp.concatenate([low, high], axis=1).reshape(2, 15, HID)
        chip = jnp.where(core == 0, chip[:, :, :HALF], chip[:, :, HALF:])
        chip = jnp.pad(chip, ((0, 0), (0, 1), (0, 0)))
        down = lax.ppermute(w_down, AX, [(64 * c + k, 2 * k + c) for c in range(2) for k in range(64)]).reshape(20, WIDTH)
        down = jnp.pad(dot(down, g_pad).astype(jnp.bfloat16), ((0, 4), (0, 0)))

        x_sib, g_sib, gates, ups, downs = gather(x_own, g_own, chip[0], chip[1], down)
        gates = gates.reshape(PAD, HALF)
        ups = ups.reshape(PAD, HALF)
        downs = downs.reshape(64, 24, PAD)[:, :20].reshape(HALF, PAD)
        h_own, da_own, du_own = activations(x_own, g_own, gates, ups, downs)
        h_sib, da_sib, du_sib = activations(x_sib, g_sib, gates, ups, downs)

        plain = dot(downs, g_pad, ((1,), (1,))).astype(jnp.bfloat16)
        y_other = lax.ppermute(dot(h_sib, plain), AX, sibling)
        y = (x_flat.astype(jnp.float32) + (dot(h_own, plain) + y_other)).astype(jnp.bfloat16).reshape(x.shape)
        d_in = dot(da_own, gates, ((1,), (1,))) + dot(du_own, ups, ((1,), (1,)))
        del d_in

        r_gate, r_up, r_down = reduce_gradients(x_own, x_sib, da_own, da_sib, du_own, du_sib, h_own, h_sib, g_own, g_sib)
        both = jnp.stack([r_gate[:15], r_up[:15]])
        other = lax.ppermute(both, AX, sibling)
        left = jnp.where(core == 0, both, other)
        right = jnp.where(core == 0, other, both)
        chip = jnp.concatenate([left, right], axis=2).reshape(2, 2, 19200)
        mine = jnp.where(core == 0, chip[:, 0], chip[:, 1])
        r_down = r_down[:, :480].reshape(2, 20, 480)
        same = jnp.where(odd == 0, r_down[0], r_down[1])
        cross = jnp.where(odd == 0, r_down[1], r_down[0])
        same = lax.ppermute(same, AX, [(2 * k + c, 64 * c + k) for c in range(2) for k in range(64)])
        cross = lax.ppermute(cross, AX, [(2 * k + c, 64 * c + (k ^ 1)) for c in range(2) for k in range(64)])
        bit = lax.axis_index(AX) % 2
        left = jnp.where(bit == 0, same, cross)
        right = jnp.where(bit == 0, cross, same)
        grad_down = jnp.concatenate([left, right], axis=1).reshape(1, 19200)
        return y, mine[0:1], mine[1:2], grad_down

    return jax.shard_map(device_step, mesh=mesh, in_specs=(row_spec, row_spec, flat_spec, flat_spec, flat_spec), out_specs=(row_spec, flat_spec, flat_spec, flat_spec), check_vma=False)
```

```python
import jax
import jax.numpy as jnp
from jax import lax
from jax.experimental import pallas as pl
from jax.experimental.pallas import tpu as pltpu
from jax.sharding import PartitionSpec as P

AX = "fsdp"
MESH = pl.DeviceIdType.MESH
N = 4
WIDTH = 960
HID = 2560
HALF = 1280
ROWS = 1024
PAD = 1024
SLOPE = 0.7978845608028654
CUBE = 0.044715
TILE = 256
BLOCK = 512
HALF_WIDTH = 480
TILES = 5
WAVES = 10
CHUNK = ((16, 256), (16, 256), (8, 512))
REDUCE_DIMS = ((0, 1, 2), (1, 2, 0), (2, 0, 1))
GATHER_DIMS = ((2, 1, 0), (1, 0, 2), (0, 2, 1))


def place():
    me = lax.axis_index(AX)
    return (me // 32, (me // 8) % 4, (me // 2) % 4), me % 2


def device(pos, core):
    return (((pos[0] * 4 + pos[1]) * 4 + pos[2]) * 2 + core,)


def shifted(pos, dim, by):
    moved = list(pos)
    moved[dim] = (pos[dim] + by + N) % N
    return tuple(moved)


def greet(pos, core):
    barrier = pltpu.get_barrier_semaphore()
    others = [device(shifted(pos, dim, by), core) for dim in range(3) for by in (1, -1)] + [device(pos, 1 - core)]
    for other in others:
        pl.semaphore_signal(barrier, inc=1, device_id=other, device_id_type=MESH)
    pl.semaphore_wait(barrier, len(others))


def gather_kernel(x_t, g_t, w_gate, w_up, w_down, x_own, x_sib, g_own, g_sib, o_gate, o_up, o_down, raw, staged, send_sem, recv_sem, pair_sem, load_sem):
    pos, core = place()
    sources = ((x_t, 0), (g_t, 0), (x_t, 1), (g_t, 1))
    targets = ((x_own, x_sib), (g_own, g_sib))
    loads = [pltpu.make_async_copy(src.at[micro], raw.at[i], load_sem.at[i]) for i, (src, micro) in enumerate(sources)]
    for c in loads:
        c.start()
    greet(pos, core)
    pieces = (w_gate, w_up, w_down)
    outs = (o_gate, o_up, o_down)
    for s in range(3):
        outs[s][pos[0], pos[1], pos[2]] = pieces[s][...]

    def block(s, phase, by):
        dims = GATHER_DIMS[s]
        index = list(shifted(pos, dims[phase], by))
        for dim in dims[:phase]:
            index[dim] = slice(None)
        return tuple(index)

    def copy(s, phase, kind, src, dst):
        to = device(shifted(pos, GATHER_DIMS[s][phase], 1 if kind % 2 == 0 else -1), core)
        return pltpu.make_async_remote_copy(src_ref=src, dst_ref=dst, send_sem=send_sem.at[s, phase, kind], recv_sem=recv_sem.at[s, phase, kind], device_id=to, device_id_type=MESH)

    def widen(i):
        loads[i].wait()
        for lane in range(0, PAD, TILE):
            col = lax.broadcasted_iota(jnp.int32, (WIDTH, TILE), 1) + lane
            row = lax.broadcasted_iota(jnp.int32, (WIDTH, TILE), 0)
            if i % 2 == 0:
                spread = (row == col - (col >> 4)) & ((col & 15) != 15)
            else:
                spread = ((row == col) & (col < 480)) | ((row == col - 32) & (col >= BLOCK))
            spread = jnp.where(spread, 1.0, 0.0).astype(jnp.bfloat16)
            for t in range(0, ROWS, BLOCK):
                r = lax.dot_general(raw[i, :, t : t + BLOCK], spread, (((0,), (0,)), ((), ())), preferred_element_type=jnp.float32)
                staged[i, t : t + BLOCK, lane : lane + TILE] = r.astype(jnp.bfloat16)

    def pass_on(i):
        own, sib = targets[i % 2]
        rows = pl.ds((i // 2) * ROWS, ROWS)
        return [
            pltpu.make_async_copy(staged.at[i], own.at[rows], pair_sem.at[0, i]),
            pltpu.make_async_remote_copy(src_ref=staged.at[i], dst_ref=sib.at[rows], send_sem=pair_sem.at[1, i], recv_sem=pair_sem.at[2, i], device_id=device(pos, 1 - core), device_id_type=MESH),
        ]

    copies = []
    for phase in range(3):
        first = []
        for s in range(3):
            mine = outs[s].at[block(s, phase, 0)]
            src = pieces[s] if phase == 0 else mine
            first.append([copy(s, phase, kind, src, mine) for kind in range(2)])
            for c in first[s]:
                c.start()
        if phase < 2:
            widen(2 * phase)
        second = []
        for s in range(3):
            lanes = outs[s].shape[-1] // 2
            row = []
            for kind in range(2):
                first[s][kind].wait_recv()
                part = outs[s].at[block(s, phase, -1 if kind == 0 else 1)]
                part = part.at[(slice(None),) * (len(part.shape) - 1) + (pl.ds(kind * lanes, lanes),)]
                row.append(copy(s, phase, 2 + kind, part, part))
                row[kind].start()
            second.append(row)
        if phase < 2:
            widen(2 * phase + 1)
        for s in range(3):
            for c in second[s]:
                c.wait_recv()
            copies += first[s] + second[s]
        if phase < 2:
            for i in (2 * phase, 2 * phase + 1):
                for c in pass_on(i):
                    c.start()
    for c in copies:
        c.wait_send()
    for i in range(4):
        for c in pass_on(i):
            c.wait()


def gather(x_t, g_t, w_gate, w_up, w_down):
    shapes = [w.shape for w in (w_gate, w_up, w_down)]
    vmem = pl.BlockSpec(memory_space=pltpu.VMEM)
    hbm = pl.BlockSpec(memory_space=pl.ANY)
    bf16 = jnp.bfloat16
    return pl.pallas_call(
        gather_kernel,
        out_shape=[jax.ShapeDtypeStruct((2 * ROWS, PAD), bf16)] * 4 + [jax.ShapeDtypeStruct((N, N, N) + s, bf16) for s in shapes],
        in_specs=[hbm] * 2 + [vmem] * 3,
        out_specs=[hbm] * 4 + [vmem] * 3,
        scratch_shapes=[
            pltpu.VMEM((4, WIDTH, ROWS), bf16),
            pltpu.VMEM((4, ROWS, PAD), bf16),
            pltpu.SemaphoreType.DMA((3, 3, 4)),
            pltpu.SemaphoreType.DMA((3, 3, 4)),
            pltpu.SemaphoreType.DMA((3, 4)),
            pltpu.SemaphoreType.DMA((4,)),
        ],
        compiler_params=pltpu.CompilerParams(collective_id=0, has_side_effects=True, vmem_limit_bytes=50 * 2**20),
        name="gather_weights",
    )(x_t, g_t, w_gate, w_up, w_down)


def reduce_kernel(x_o, x_s, g_o, g_s, x_t, w_gate, w_up, w_down, out_g, out_u, out_d, h_o, h_s, y_t, y_in, *scratch):
    xv, gv, wg, wu, wd, hv, dav, duv = scratch[:8]
    part = scratch[8:11]
    line = scratch[11:14]
    point = scratch[14:17]
    inbox = [scratch[17 + 6 * s : 23 + 6 * s] for s in range(3)]
    send_sem, recv_sem, keep_sem, weight_sem, out_sem, back_sem, x_sem, y_send, y_recv, y_load, y_out, xy, y_part, y_other, wt = scratch[35:]
    outs = (out_g, out_u, out_d)
    pos, core = place()

    def keep(micro):
        rows = pl.ds(micro * ROWS, ROWS)
        return [pltpu.make_async_copy(src.at[rows], dst.at[micro, pl.ds(i * ROWS, ROWS)], keep_sem.at[micro, kind, i]) for kind, (both, dst) in enumerate((((x_o, x_s), xv), ((g_o, g_s), gv))) for i, src in enumerate(both)]

    weights = [pltpu.make_async_copy(src, dst, weight_sem.at[i]) for i, (src, dst) in enumerate(((w_gate, wg), (w_up, wu), (w_down, wd)))]
    x_loads = [pltpu.make_async_copy(x_t.at[m], xy, x_sem.at[m]) for m in range(2)]
    for c in weights + keep(0) + keep(1) + x_loads[:1]:
        c.start()
    greet(pos, core)

    def hidden_out(wave):
        rows = pl.ds(pl.multiple_of((wave // TILES) * ROWS, ROWS), ROWS)
        lanes = pl.ds(pl.multiple_of((wave % TILES) * TILE, TILE), TILE)
        return [pltpu.make_async_copy(hv.at[wave % 2, pl.ds(i * ROWS, ROWS)], dst.at[rows, lanes], out_sem.at[wave % 2, i]) for i, dst in enumerate((h_o, h_s))]

    def half(s, phase, way):
        if phase == 2:
            lanes = CHUNK[s][1] // 2
            return pl.ds(lanes * (1 - way), lanes)
        return pl.ds(2 * (1 - way), 2)

    def send(s, kind, way, wave):
        dims = REDUCE_DIMS[s]
        phase, step = kind // 2, kind % 2
        dim = dims[phase]
        rest = [d for d in range(3) if d not in dims[:phase]]
        buf = (part, line, point)[phase][s].at[wave % 3]
        dest = (pos[dim] + (2 if step == 0 else (1 if way == 0 else 3))) % N
        index = [slice(None)] * len(rest)
        index[rest.index(dim)] = dest
        src = buf.at[tuple(index)]
        if step == 0:
            src = src.at[(slice(None), half(s, phase, way))] if phase == 2 else src.at[half(s, phase, way)]
        to = device(shifted(pos, dim, 1 if way == 0 else -1), core)
        return pltpu.make_async_remote_copy(src_ref=src, dst_ref=inbox[s][kind].at[wave % 4, way], send_sem=send_sem.at[s, kind, way, wave % 4], recv_sem=recv_sem.at[s, kind, way, wave % 4], device_id=to, device_id_type=MESH)

    def activate(wave):
        micro, n = wave // TILES, wave % TILES
        lanes = pl.ds(pl.multiple_of(n * TILE, TILE), TILE)

        @pl.loop(0, 4)
        def _(i):
            rows = pl.ds(pl.multiple_of(i * BLOCK, BLOCK), BLOCK)
            x_in, d_out = xv[micro, rows, :], gv[micro, rows, :]
            a = dot(x_in, wg[:, lanes]).astype(jnp.bfloat16).astype(jnp.float32)
            u = dot(x_in, wu[:, lanes]).astype(jnp.bfloat16).astype(jnp.float32)
            dh = dot(d_out, wd[lanes, :], ((1,), (1,))).astype(jnp.bfloat16).astype(jnp.float32)
            squared = a * a
            t = jnp.tanh(SLOPE * (a + CUBE * (squared * a)))
            cdf = 0.5 * (1.0 + t)
            gelu = a * cdf
            slope = cdf + (0.5 * a) * (1.0 - t * t) * (SLOPE * (1.0 + (3.0 * CUBE) * squared))
            hv[wave % 2, rows, :] = (gelu * u).astype(jnp.bfloat16)
            dav[rows, :] = (dh * u * slope).astype(jnp.bfloat16)
            duv[rows, :] = (dh * gelu).astype(jnp.bfloat16)

    def across_rows(a, b):
        return lax.dot_general(a, b, (((0,), (0,)), ((), ())), preferred_element_type=jnp.float32)

    def products(wave):
        micro = wave // TILES
        for s, d in ((0, dav), (1, duv)):
            for i in range(2):
                r = across_rows(xv[micro, :, i * BLOCK : i * BLOCK + BLOCK], d[...])
                part[s][wave % 3, 2 * i : 2 * i + 2] = r.reshape(2, N, N, 16, TILE)
        for j in range(2):
            r = across_rows(hv[wave % 2], gv[micro, :, j * BLOCK : j * BLOCK + BLOCK]).reshape(N, N, 2, 8, BLOCK)
            for m in range(2):
                part[2][wave % 3, :, :, 2 * m + j] = r[:, :, m]

    def stage(s, step, wave):
        if step > 0:
            kind = step - 1
            phase = kind // 2
            dims = REDUCE_DIMS[s]
            dim = dims[phase]
            rest = [d for d in range(3) if d not in dims[:phase]]
            at = rest.index(dim)
            buf = (part, line, point)[phase][s]
            arrived = inbox[s][kind]
            for way in range(2):
                send(s, kind, way, wave).wait_recv()
            if kind % 2 == 0:
                for way in range(2):
                    index = [slice(None)] * len(rest)
                    index[at] = (pos[dim] + (1 if way == 0 else 3)) % N
                    if phase == 2:
                        index += [slice(None), half(s, phase, way)]
                    else:
                        index[[i for i in range(len(rest)) if i != at][0]] = half(s, phase, way)
                    buf[tuple([wave % 3] + index)] += arrived[wave % 4, way]
            else:
                index = [slice(None)] * len(rest)
                index[at] = pos[dim]
                total = buf[tuple([wave % 3] + index)] + arrived[wave % 4, 0] + arrived[wave % 4, 1]
                for way in range(2):
                    send(s, kind - 1, way, wave).wait_send()
                    send(s, kind, way, wave).wait_send()
                if phase < 2:
                    (line, point)[phase][s][wave % 3] = total
                else:
                    micro, n = wave // TILES, wave % TILES
                    if s < 2:
                        spot = (slice(None), pl.ds(pl.multiple_of(n * TILE, TILE), TILE))
                    else:
                        spot = (pl.ds(pl.multiple_of(n * 8, 8), 8), slice(None))

                    @pl.when(micro == 0)
                    def _():
                        outs[s][spot] = total

                    @pl.when(micro == 1)
                    def _():
                        outs[s][spot] += total
        if step < 6:
            for way in range(2):
                send(s, step, way, wave).start()

    def hidden_back(m):
        rows = pl.ds(m * ROWS, ROWS)
        return [
            pltpu.make_async_copy(src.at[rows, pl.ds(lane, wide)], dst.at[m, pl.ds(i * ROWS, ROWS), pl.ds(0, wide)], back_sem.at[m, k, i])
            for i, src in enumerate((h_o, h_s))
            for k, (dst, lane, wide) in enumerate(((xv, 0, PAD), (gv, PAD, HALF - PAD)))
        ]

    def y_rows(m, who, i, j):
        rows = slice(who * ROWS + TILE * i, who * ROWS + TILE * i + TILE)
        cols = slice(BLOCK * j, BLOCK * j + HALF_WIDTH)
        return dot(wt[cols, :PAD], xv[m, rows, :], ((1,), (1,))) + dot(wt[cols, PAD:], gv[m, rows, : HALF - PAD], ((1,), (1,)))

    def y_hand(m, i):
        return pltpu.make_async_remote_copy(src_ref=y_part.at[i % 2], dst_ref=y_in.at[m, :, pl.ds(TILE * i, TILE)], send_sem=y_send.at[m, i], recv_sem=y_recv.at[m, i], device_id=device(pos, 1 - core), device_id_type=MESH)

    def y_fetch(m, i):
        return pltpu.make_async_copy(y_in.at[m, :, pl.ds(TILE * i, TILE)], y_other.at[i % 2], y_load.at[m, i])

    def y_done(m, i):
        lanes = pl.ds(TILE * i, TILE)
        return pltpu.make_async_copy(xy.at[:, lanes], y_t.at[m, :, lanes], y_out.at[m, i])

    def y_for_sibling(m):
        for i in range(4):
            if i >= 2:
                y_hand(m, i - 2).wait_send()
            for j in range(2):
                y_part[i % 2, HALF_WIDTH * j : HALF_WIDTH * j + HALF_WIDTH, :] = y_rows(m, 1, i, j)
            y_hand(m, i).start()

    def y_own(m):
        for i in range(2, 4):
            y_hand(m, i).wait_send()
        for i in range(2):
            y_hand(m, i).wait_recv()
            y_fetch(m, i).start()
        for i in range(4):
            y_fetch(m, i).wait()
            for j in range(2):
                part = slice(HALF_WIDTH * j, HALF_WIDTH * j + HALF_WIDTH)
                lanes = slice(TILE * i, TILE * i + TILE)
                total = y_rows(m, 0, i, j) + y_other[i % 2, part, :]
                xy[part, lanes] = (xy[part, lanes].astype(jnp.float32) + total).astype(jnp.bfloat16)
            if i < 2:
                y_hand(m, i + 2).wait_recv()
                y_fetch(m, i + 2).start()
            y_done(m, i).start()

    for c in weights:
        c.wait()

    @pl.loop(0, WAVES + 6)
    def _(slot):
        for micro in range(2):

            @pl.when(slot == micro * TILES)
            def _():
                for c in keep(micro):
                    c.wait()

        @pl.when((slot >= 2) & (slot < WAVES + 2))
        def _():
            for c in hidden_out(slot - 2):
                c.wait()

        @pl.when(slot < WAVES)
        def _():
            activate(slot)
            products(slot)
            for c in hidden_out(slot):
                c.start()

        for step in range(7):

            @pl.when((slot >= step) & (slot - step < WAVES))
            def _():
                for s in range(3):
                    stage(s, step, slot - step)

        @pl.when(slot == 6)
        def _():
            for c in hidden_back(0):
                c.start()
            for i in range(TILES):
                wt[:, i * TILE : i * TILE + TILE] = wd[i * TILE : i * TILE + TILE, :].T

        @pl.when(slot == 7)
        def _():
            for c in hidden_back(0):
                c.wait()
            y_for_sibling(0)

        @pl.when(slot == 11)
        def _():
            for c in hidden_back(1):
                c.start()

        @pl.when(slot == 12)
        def _():
            for i in range(4):
                y_done(0, i).wait()
            x_loads[1].start()
            for c in hidden_back(1):
                c.wait()
            y_for_sibling(1)

        for m in range(2):

            @pl.when(slot == 9 + 5 * m)
            def _():
                x_loads[m].wait()
                y_own(m)

    for i in range(4):
        y_done(1, i).wait()


def reduce_gradients(*operands):
    hbm = pl.BlockSpec(memory_space=pl.ANY)
    vmem = pl.BlockSpec(memory_space=pltpu.VMEM)
    f32 = jnp.float32
    bf16 = jnp.bfloat16
    scratch = [pltpu.VMEM((2, 2 * ROWS, PAD), bf16)] * 2
    scratch += [pltpu.VMEM((PAD, HALF), bf16)] * 2 + [pltpu.VMEM((HALF, PAD), bf16)]
    scratch += [pltpu.VMEM((2, 2 * ROWS, TILE), bf16)] + [pltpu.VMEM((2 * ROWS, TILE), bf16)] * 2
    scratch += [pltpu.VMEM((3, N, N, N) + CHUNK[s], f32) for s in range(3)]
    scratch += [pltpu.VMEM((3, N, N) + CHUNK[s], f32) for s in range(3)]
    scratch += [pltpu.VMEM((3, N) + CHUNK[s], f32) for s in range(3)]
    for s in range(3):
        rows, lanes = CHUNK[s]
        scratch += [pltpu.VMEM((4, 2) + lead + CHUNK[s], f32) for lead in ((2, N), (N, N), (2,), (N,))]
        scratch += [pltpu.VMEM((4, 2, rows, lanes // 2), f32), pltpu.VMEM((4, 2) + CHUNK[s], f32)]
    scratch += [pltpu.SemaphoreType.DMA((3, 6, 2, 4)), pltpu.SemaphoreType.DMA((3, 6, 2, 4)), pltpu.SemaphoreType.DMA((2, 2, 2)), pltpu.SemaphoreType.DMA((3,)), pltpu.SemaphoreType.DMA((2, 2))]
    scratch += [pltpu.SemaphoreType.DMA((2, 2, 2)), pltpu.SemaphoreType.DMA((2,))] + [pltpu.SemaphoreType.DMA((2, 4))] * 4
    scratch += [pltpu.VMEM((WIDTH, ROWS), bf16), pltpu.VMEM((2, WIDTH, TILE), f32), pltpu.VMEM((2, WIDTH, TILE), f32), pltpu.VMEM((PAD, HALF), bf16)]
    return pl.pallas_call(
        reduce_kernel,
        out_shape=[jax.ShapeDtypeStruct((16, HALF), f32), jax.ShapeDtypeStruct((16, HALF), f32), jax.ShapeDtypeStruct((40, BLOCK), f32)] + [jax.ShapeDtypeStruct((2 * ROWS, HALF), bf16)] * 2 + [jax.ShapeDtypeStruct((2, WIDTH, ROWS), bf16), jax.ShapeDtypeStruct((2, WIDTH, ROWS), f32)],
        in_specs=[hbm] * 8,
        out_specs=[vmem] * 3 + [hbm] * 4,
        scratch_shapes=scratch,
        compiler_params=pltpu.CompilerParams(collective_id=1, has_side_effects=True, vmem_limit_bytes=63 * 2**20),
        name="reduce_gradients",
    )(*operands)


def gelu_tanh(z):
    return jax.nn.gelu(z, approximate=True)


def dot(a, b, dims=((1,), (0,))):
    return lax.dot_general(a, b, (dims, ((), ())), preferred_element_type=jnp.float32)


def activations(x_in, d_out, gate_w, up_w, down_w):
    pre_gate = dot(x_in, gate_w).astype(jnp.bfloat16)
    pre_up = dot(x_in, up_w).astype(jnp.bfloat16)
    up_float = pre_up.astype(jnp.float32)
    gelu_val, gelu_vjp = jax.vjp(gelu_tanh, pre_gate.astype(jnp.float32))
    hidden = (gelu_val * up_float).astype(jnp.bfloat16)
    d_hidden = dot(d_out, down_w, ((1,), (1,))).astype(jnp.bfloat16).astype(jnp.float32)
    d_gate = gelu_vjp(d_hidden * up_float)[0].astype(jnp.bfloat16)
    d_up = (d_hidden * gelu_val).astype(jnp.bfloat16)
    return hidden, d_gate, d_up


def solution(mesh):
    row_spec = P(None, AX, None)
    flat_spec = P(None, AX)
    sibling = [(i, i ^ 1) for i in range(128)]

    def shuffle(dtype):
        row = lax.broadcasted_iota(jnp.int32, (HALF, HALF), 0)
        col = lax.broadcasted_iota(jnp.int32, (HALF, HALF), 1)
        return (row == ((col // 8) % 32) * 40 + (col // TILE) * 8 + col % 8).astype(dtype)

    def device_step(x, g, w_gate, w_up, w_down):
        core = lax.axis_index(AX) % 2
        odd = (lax.axis_index(AX) // 2) % 2
        both = jnp.concatenate([w_gate, w_up], axis=0)
        other = lax.ppermute(both, AX, sibling)
        low = jnp.where(core == 0, both, other)
        high = jnp.where(core == 0, other, both)
        chip = jnp.concatenate([low, high], axis=1).reshape(2, 15, HID)
        chip = jnp.where(core == 0, chip[:, :, :HALF], chip[:, :, HALF:])
        chip = dot(jnp.pad(chip, ((0, 0), (0, 1), (0, 0))).reshape(32, HALF), shuffle(jnp.bfloat16)).astype(jnp.bfloat16).reshape(2, 16, HALF)
        down = lax.ppermute(w_down, AX, [(64 * c + k, 2 * k + c) for c in range(2) for k in range(64)]).reshape(20, WIDTH)
        down = jnp.pad(down.reshape(20, 2, HALF_WIDTH), ((0, 4), (0, 0), (0, 32))).reshape(24, PAD)

        x_t = x.transpose(0, 2, 1)
        g_t = g.transpose(0, 2, 1)
        x_own, x_sib, g_own, g_sib, gates, ups, downs = gather(x_t, g_t, chip[0], chip[1], down)
        gates = gates.reshape(PAD, HALF)
        ups = ups.reshape(PAD, HALF)
        downs = downs.reshape(64, 24, PAD)[:, :20].reshape(32, 5, 8, PAD).transpose(1, 0, 2, 3).reshape(HALF, PAD)
        r_gate, r_up, r_down, _, _, y_t, _ = reduce_gradients(x_own, x_sib, g_own, g_sib, x_t, gates, ups, downs)
        y = y_t.transpose(0, 2, 1)

        da_own, du_own = activations(x_own, g_own, gates, ups, downs)[1:]
        d_in = dot(da_own, gates, ((1,), (1,))) + dot(du_own, ups, ((1,), (1,)))
        del d_in

        both = jnp.concatenate([r_gate, r_up])
        both = lax.dot_general(both, shuffle(jnp.float32), (((1,), (1,)), ((), ())), precision=lax.Precision.HIGHEST, preferred_element_type=jnp.float32)
        both = both.reshape(2, 16, HALF)[:, :15]
        other = lax.ppermute(both, AX, sibling)
        left = jnp.where(core == 0, both, other)
        right = jnp.where(core == 0, other, both)
        chip = jnp.concatenate([left, right], axis=2).reshape(2, 2, 19200)
        mine = jnp.where(core == 0, chip[:, 0], chip[:, 1])
        r_down = r_down[:, :HALF_WIDTH].reshape(2, 20, HALF_WIDTH)
        same = jnp.where(odd == 0, r_down[0], r_down[1])
        cross = jnp.where(odd == 0, r_down[1], r_down[0])
        same = lax.ppermute(same, AX, [(2 * k + c, 64 * c + k) for c in range(2) for k in range(64)])
        cross = lax.ppermute(cross, AX, [(2 * k + c, 64 * c + (k ^ 1)) for c in range(2) for k in range(64)])
        bit = lax.axis_index(AX) % 2
        left = jnp.where(bit == 0, same, cross)
        right = jnp.where(bit == 0, cross, same)
        grad_down = jnp.concatenate([left, right], axis=1).reshape(1, 19200)
        return y, mine[0:1], mine[1:2], grad_down

    return jax.shard_map(device_step, mesh=mesh, in_specs=(row_spec, row_spec, flat_spec, flat_spec, flat_spec), out_specs=(row_spec, flat_spec, flat_spec, flat_spec), check_vma=False)
```

```python
import jax
import jax.numpy as jnp
from jax import lax
from jax.experimental import pallas as pl
from jax.experimental.pallas import tpu as pltpu
from jax.sharding import PartitionSpec as P

AX = "fsdp"
MESH = pl.DeviceIdType.MESH
N = 4
WIDTH = 960
HID = 2560
HALF = 1280
ROWS = 1024
PAD = 1024
SLOPE = 0.7978845608028654
CUBE = 0.044715
TILE = 256
BLOCK = 512
HALF_WIDTH = 480
TILES = 5
WAVES = 10
LEAD = 6
CHUNK = ((16, 256), (16, 256), (8, 512))
REDUCE_DIMS = ((0, 1, 2), (1, 2, 0), (2, 0, 1))
GATHER_DIMS = ((2, 1, 0), (1, 0, 2), (0, 2, 1))


def place():
    me = lax.axis_index(AX)
    return (me // 32, (me // 8) % 4, (me // 2) % 4), me % 2


def device(pos, core):
    return (((pos[0] * 4 + pos[1]) * 4 + pos[2]) * 2 + core,)


def shifted(pos, dim, by):
    moved = list(pos)
    moved[dim] = (pos[dim] + by + N) % N
    return tuple(moved)


def greet(pos, core):
    barrier = pltpu.get_barrier_semaphore()
    others = [device(shifted(pos, dim, by), core) for dim in range(3) for by in (1, -1)] + [device(pos, 1 - core)]
    for other in others:
        pl.semaphore_signal(barrier, inc=1, device_id=other, device_id_type=MESH)
    pl.semaphore_wait(barrier, len(others))


def step_kernel(x_t, g_t, w_gate, w_up, w_down, out_g, out_u, out_d, h_o, h_s, y_t, y_in, *scratch):
    xv, gv, wg, wu, wd, hv, dav, duv = scratch[:8]
    part = scratch[8:11]
    line = scratch[11:14]
    point = scratch[14:17]
    inbox = [scratch[17 + 6 * s : 23 + 6 * s] for s in range(3)]
    send_sem, recv_sem, keep_sem, out_sem, back_sem, x_sem, y_send, y_recv, y_load, y_out, xy, y_part, y_other, wt, gather_send, gather_recv = scratch[35:]
    outs = (out_g, out_u, out_d)
    pos, core = place()

    wide = ((x_t, xv, 0), (g_t, gv, 0), (x_t, xv, 1), (g_t, gv, 1))
    weights = (wg, wu, wd)

    def raw(i):
        return pltpu.make_async_copy(wide[i][0].at[wide[i][2]], xy, keep_sem.at[0, i])

    def pair(i):
        buf = wide[i][1].at[wide[i][2]]
        return pltpu.make_async_remote_copy(src_ref=buf.at[pl.ds(0, ROWS)], dst_ref=buf.at[pl.ds(ROWS, ROWS)], send_sem=keep_sem.at[1, i], recv_sem=keep_sem.at[2, i], device_id=device(pos, 1 - core), device_id_type=MESH)

    def widen(i):
        buf, micro = wide[i][1:]
        for lane in range(0, PAD, TILE):
            col = lax.broadcasted_iota(jnp.int32, (WIDTH, TILE), 1) + lane
            row = lax.broadcasted_iota(jnp.int32, (WIDTH, TILE), 0)
            if i % 2 == 0:
                spread = (row == col - (col >> 4)) & ((col & 15) != 15)
            else:
                spread = ((row == col) & (col < HALF_WIDTH)) | ((row == col - 32) & (col >= BLOCK))
            spread = jnp.where(spread, 1.0, 0.0).astype(jnp.bfloat16)
            for t in range(0, ROWS, BLOCK):
                buf[micro, t : t + BLOCK, lane : lane + TILE] = across_rows(xy[:, t : t + BLOCK], spread).astype(jnp.bfloat16)

    def piece(s, n):
        if s == 2:
            return w_down.at[n]
        return (w_gate, w_up)[s].at[:, pl.ds(pl.multiple_of(n * TILE, TILE), TILE)]

    def gather_copy(s, phase, kind, n):
        dims = GATHER_DIMS[s]
        by = 0 if kind < 2 else (-1 if kind == 2 else 1)
        index = list(shifted(pos, dims[phase], by))
        for dim in dims[:phase]:
            index[dim] = slice(None)
        dst = weights[s].at[tuple([n] + index)]
        src = dst
        if kind >= 2:
            lanes = TILE // 2
            dst = dst.at[(slice(None),) * (len(dst.shape) - 1) + (pl.ds((kind - 2) * lanes, lanes),)]
            src = dst
        elif phase == 0:
            src = piece(s, n)
        to = device(shifted(pos, dims[phase], 1 if kind % 2 == 0 else -1), core)
        return pltpu.make_async_remote_copy(src_ref=src, dst_ref=dst, send_sem=gather_send.at[s, phase, kind, n], recv_sem=gather_recv.at[s, phase, kind, n], device_id=to, device_id_type=MESH)

    def gather_step(s, step, n):
        phase = step // 2
        if step % 2 == 1:
            for kind in range(2):
                gather_copy(s, phase, kind, n).wait_recv()
                gather_copy(s, phase, kind + 2, n).start()
            return
        if step > 0:
            for kind in range(2, 4):
                gather_copy(s, phase - 1, kind, n).wait_recv()
        if step < 6:
            for kind in range(2):
                gather_copy(s, phase, kind, n).start()
        else:
            for p in range(3):
                for kind in range(4):
                    gather_copy(s, p, kind, n).wait_send()

    x_loads = [pltpu.make_async_copy(x_t.at[m], xy, x_sem.at[m]) for m in range(2)]
    raw(0).start()
    greet(pos, core)
    for s in range(3):
        for n in range(TILES):
            own = w_down[n] if s == 2 else (w_gate, w_up)[s][:, n * TILE : n * TILE + TILE]
            weights[s][n, pos[0], pos[1], pos[2]] = own

    def hidden_out(wave):
        rows = pl.ds(pl.multiple_of((wave // TILES) * ROWS, ROWS), ROWS)
        lanes = pl.ds(pl.multiple_of((wave % TILES) * TILE, TILE), TILE)
        return [pltpu.make_async_copy(hv.at[wave % 2, pl.ds(i * ROWS, ROWS)], dst.at[rows, lanes], out_sem.at[wave % 2, i]) for i, dst in enumerate((h_o, h_s))]

    def half(s, phase, way):
        if phase == 2:
            lanes = CHUNK[s][1] // 2
            return pl.ds(lanes * (1 - way), lanes)
        return pl.ds(2 * (1 - way), 2)

    def send(s, kind, way, wave):
        dims = REDUCE_DIMS[s]
        phase, step = kind // 2, kind % 2
        dim = dims[phase]
        rest = [d for d in range(3) if d not in dims[:phase]]
        buf = (part, line, point)[phase][s].at[wave % 3]
        dest = (pos[dim] + (2 if step == 0 else (1 if way == 0 else 3))) % N
        index = [slice(None)] * len(rest)
        index[rest.index(dim)] = dest
        src = buf.at[tuple(index)]
        if step == 0:
            src = src.at[(slice(None), half(s, phase, way))] if phase == 2 else src.at[half(s, phase, way)]
        to = device(shifted(pos, dim, 1 if way == 0 else -1), core)
        return pltpu.make_async_remote_copy(src_ref=src, dst_ref=inbox[s][kind].at[wave % 4, way], send_sem=send_sem.at[s, kind, way, wave % 4], recv_sem=recv_sem.at[s, kind, way, wave % 4], device_id=to, device_id_type=MESH)

    def activate(wave):
        micro, n = wave // TILES, wave % TILES

        @pl.loop(0, 4)
        def _(i):
            rows = pl.ds(pl.multiple_of(i * BLOCK, BLOCK), BLOCK)
            x_in, d_out = xv[micro, rows, :], gv[micro, rows, :]
            a = dot(x_in, wg[n].reshape(PAD, TILE)).astype(jnp.bfloat16).astype(jnp.float32)
            u = dot(x_in, wu[n].reshape(PAD, TILE)).astype(jnp.bfloat16).astype(jnp.float32)
            dh = sum(dot(d_out[:, q * TILE : q * TILE + TILE], wd[n, :, :, q].reshape(TILE, TILE), ((1,), (1,))) for q in range(N)).astype(jnp.bfloat16).astype(jnp.float32)
            squared = a * a
            t = jnp.tanh(SLOPE * (a + CUBE * (squared * a)))
            cdf = 0.5 * (1.0 + t)
            gelu = a * cdf
            slope = cdf + (0.5 * a) * (1.0 - t * t) * (SLOPE * (1.0 + (3.0 * CUBE) * squared))
            hv[wave % 2, rows, :] = (gelu * u).astype(jnp.bfloat16)
            dav[rows, :] = (dh * u * slope).astype(jnp.bfloat16)
            duv[rows, :] = (dh * gelu).astype(jnp.bfloat16)

    def across_rows(a, b):
        return lax.dot_general(a, b, (((0,), (0,)), ((), ())), preferred_element_type=jnp.float32)

    def products(wave):
        micro = wave // TILES
        for s, d in ((0, dav), (1, duv)):
            for i in range(2):
                r = across_rows(xv[micro, :, i * BLOCK : i * BLOCK + BLOCK], d[...])
                part[s][wave % 3, 2 * i : 2 * i + 2] = r.reshape(2, N, N, 16, TILE)
        for j in range(2):
            r = across_rows(hv[wave % 2], gv[micro, :, j * BLOCK : j * BLOCK + BLOCK]).reshape(N, N, 2, 8, BLOCK)
            for m in range(2):
                part[2][wave % 3, :, :, 2 * m + j] = r[:, :, m]

    def stage(s, step, wave):
        if step > 0:
            kind = step - 1
            phase = kind // 2
            dims = REDUCE_DIMS[s]
            dim = dims[phase]
            rest = [d for d in range(3) if d not in dims[:phase]]
            at = rest.index(dim)
            buf = (part, line, point)[phase][s]
            arrived = inbox[s][kind]
            for way in range(2):
                send(s, kind, way, wave).wait_recv()
            if kind % 2 == 0:
                for way in range(2):
                    index = [slice(None)] * len(rest)
                    index[at] = (pos[dim] + (1 if way == 0 else 3)) % N
                    if phase == 2:
                        index += [slice(None), half(s, phase, way)]
                    else:
                        index[[i for i in range(len(rest)) if i != at][0]] = half(s, phase, way)
                    buf[tuple([wave % 3] + index)] += arrived[wave % 4, way]
            else:
                index = [slice(None)] * len(rest)
                index[at] = pos[dim]
                total = buf[tuple([wave % 3] + index)] + arrived[wave % 4, 0] + arrived[wave % 4, 1]
                for way in range(2):
                    send(s, kind - 1, way, wave).wait_send()
                    send(s, kind, way, wave).wait_send()
                if phase < 2:
                    (line, point)[phase][s][wave % 3] = total
                else:
                    micro, n = wave // TILES, wave % TILES
                    if s < 2:
                        spot = (slice(None), pl.ds(pl.multiple_of(n * TILE, TILE), TILE))
                    else:
                        spot = (pl.ds(pl.multiple_of(n * 8, 8), 8), slice(None))

                    @pl.when(micro == 0)
                    def _():
                        outs[s][spot] = total

                    @pl.when(micro == 1)
                    def _():
                        outs[s][spot] += total
        if step < 6:
            for way in range(2):
                send(s, step, way, wave).start()

    def hidden_back(m):
        rows = pl.ds(m * ROWS, ROWS)
        return [
            pltpu.make_async_copy(src.at[rows, pl.ds(lane, wide)], dst.at[m, pl.ds(i * ROWS, ROWS), pl.ds(0, wide)], back_sem.at[m, k, i])
            for i, src in enumerate((h_o, h_s))
            for k, (dst, lane, wide) in enumerate(((xv, 0, PAD), (gv, PAD, HALF - PAD)))
        ]

    def y_rows(m, who, i, j):
        rows = slice(who * ROWS + TILE * i, who * ROWS + TILE * i + TILE)
        cols = slice(BLOCK * j, BLOCK * j + HALF_WIDTH)
        return dot(wt[cols, :PAD], xv[m, rows, :], ((1,), (1,))) + dot(wt[cols, PAD:], gv[m, rows, : HALF - PAD], ((1,), (1,)))

    def y_hand(m, i):
        return pltpu.make_async_remote_copy(src_ref=y_part.at[i % 2], dst_ref=y_in.at[m, :, pl.ds(TILE * i, TILE)], send_sem=y_send.at[m, i], recv_sem=y_recv.at[m, i], device_id=device(pos, 1 - core), device_id_type=MESH)

    def y_fetch(m, i):
        return pltpu.make_async_copy(y_in.at[m, :, pl.ds(TILE * i, TILE)], y_other.at[i % 2], y_load.at[m, i])

    def y_done(m, i):
        lanes = pl.ds(TILE * i, TILE)
        return pltpu.make_async_copy(xy.at[:, lanes], y_t.at[m, :, lanes], y_out.at[m, i])

    def y_for_sibling(m):
        for i in range(4):
            if i >= 2:
                y_hand(m, i - 2).wait_send()
            for j in range(2):
                y_part[i % 2, HALF_WIDTH * j : HALF_WIDTH * j + HALF_WIDTH, :] = y_rows(m, 1, i, j)
            y_hand(m, i).start()

    def y_own(m):
        for i in range(2, 4):
            y_hand(m, i).wait_send()
        for i in range(2):
            y_hand(m, i).wait_recv()
            y_fetch(m, i).start()
        for i in range(4):
            y_fetch(m, i).wait()
            for j in range(2):
                part = slice(HALF_WIDTH * j, HALF_WIDTH * j + HALF_WIDTH)
                lanes = slice(TILE * i, TILE * i + TILE)
                total = y_rows(m, 0, i, j) + y_other[i % 2, part, :]
                xy[part, lanes] = (xy[part, lanes].astype(jnp.float32) + total).astype(jnp.bfloat16)
            if i < 2:
                y_hand(m, i + 2).wait_recv()
                y_fetch(m, i + 2).start()
            y_done(m, i).start()

    @pl.loop(0, LEAD + WAVES + 6)
    def _(turn):
        slot = turn - LEAD

        for step in reversed(range(7)):

            @pl.when((turn >= step) & (turn - step < TILES))
            def _():
                for s in range(3):
                    gather_step(s, step, turn - step)

        for i in range(5):

            @pl.when(turn == i)
            def _():
                if i > 0:
                    pair(i - 1).start()
                if i < 4:
                    raw(i).wait()
                    widen(i)
                if i < 3:
                    raw(i + 1).start()
                if i == 4:
                    x_loads[0].start()

        for micro in range(2):

            @pl.when(slot == micro * TILES)
            def _():
                for i in range(2):
                    pair(2 * micro + i).wait()

        @pl.when((slot >= 2) & (slot < WAVES + 2))
        def _():
            for c in hidden_out(slot - 2):
                c.wait()

        @pl.when((slot >= 0) & (slot < WAVES))
        def _():
            activate(slot)
            products(slot)
            for c in hidden_out(slot):
                c.start()

        for step in range(7):

            @pl.when((slot >= step) & (slot - step < WAVES))
            def _():
                for s in range(3):
                    stage(s, step, slot - step)

        @pl.when(slot == 6)
        def _():
            for c in hidden_back(0):
                c.start()
            for i in range(TILES):
                for q in range(N):
                    wt[q * TILE : q * TILE + TILE, i * TILE : i * TILE + TILE] = wd[i, :, :, q].reshape(TILE, TILE).T

        @pl.when(slot == 7)
        def _():
            for c in hidden_back(0):
                c.wait()
            y_for_sibling(0)

        @pl.when(slot == 11)
        def _():
            for c in hidden_back(1):
                c.start()

        @pl.when(slot == 12)
        def _():
            for i in range(4):
                y_done(0, i).wait()
            x_loads[1].start()
            for c in hidden_back(1):
                c.wait()
            y_for_sibling(1)

        for m in range(2):

            @pl.when(slot == 9 + 5 * m)
            def _():
                x_loads[m].wait()
                y_own(m)

    for i in range(4):
        y_done(1, i).wait()


def step_on_chip(*operands):
    hbm = pl.BlockSpec(memory_space=pl.ANY)
    vmem = pl.BlockSpec(memory_space=pltpu.VMEM)
    f32 = jnp.float32
    bf16 = jnp.bfloat16
    scratch = [pltpu.VMEM((2, 2 * ROWS, PAD), bf16)] * 2
    scratch += [pltpu.VMEM((TILES, N, N, N, 16, TILE), bf16)] * 3
    scratch += [pltpu.VMEM((2, 2 * ROWS, TILE), bf16)] + [pltpu.VMEM((2 * ROWS, TILE), bf16)] * 2
    scratch += [pltpu.VMEM((3, N, N, N) + CHUNK[s], f32) for s in range(3)]
    scratch += [pltpu.VMEM((3, N, N) + CHUNK[s], f32) for s in range(3)]
    scratch += [pltpu.VMEM((3, N) + CHUNK[s], f32) for s in range(3)]
    for s in range(3):
        rows, lanes = CHUNK[s]
        scratch += [pltpu.VMEM((4, 2) + lead + CHUNK[s], f32) for lead in ((2, N), (N, N), (2,), (N,))]
        scratch += [pltpu.VMEM((4, 2, rows, lanes // 2), f32), pltpu.VMEM((4, 2) + CHUNK[s], f32)]
    scratch += [pltpu.SemaphoreType.DMA((3, 6, 2, 4)), pltpu.SemaphoreType.DMA((3, 6, 2, 4)), pltpu.SemaphoreType.DMA((3, 4)), pltpu.SemaphoreType.DMA((2, 2))]
    scratch += [pltpu.SemaphoreType.DMA((2, 2, 2)), pltpu.SemaphoreType.DMA((2,))] + [pltpu.SemaphoreType.DMA((2, 4))] * 4
    scratch += [pltpu.VMEM((WIDTH, ROWS), bf16), pltpu.VMEM((2, WIDTH, TILE), f32), pltpu.VMEM((2, WIDTH, TILE), f32), pltpu.VMEM((PAD, HALF), bf16), pltpu.SemaphoreType.DMA((3, 3, 4, TILES)), pltpu.SemaphoreType.DMA((3, 3, 4, TILES))]
    return pl.pallas_call(
        step_kernel,
        out_shape=[jax.ShapeDtypeStruct((16, HALF), f32), jax.ShapeDtypeStruct((16, HALF), f32), jax.ShapeDtypeStruct((40, BLOCK), f32)] + [jax.ShapeDtypeStruct((2 * ROWS, HALF), bf16)] * 2 + [jax.ShapeDtypeStruct((2, WIDTH, ROWS), bf16), jax.ShapeDtypeStruct((2, WIDTH, ROWS), f32)],
        in_specs=[hbm] * 2 + [vmem] * 3,
        out_specs=[vmem] * 3 + [hbm] * 4,
        scratch_shapes=scratch,
        compiler_params=pltpu.CompilerParams(collective_id=0, has_side_effects=True, vmem_limit_bytes=63 * 2**20),
        name="mlp_step",
    )(*operands)


def gelu_tanh(z):
    return jax.nn.gelu(z, approximate=True)


def dot(a, b, dims=((1,), (0,))):
    return lax.dot_general(a, b, (dims, ((), ())), preferred_element_type=jnp.float32)


def activations(x_in, d_out, gate_w, up_w, down_w):
    pre_gate = dot(x_in, gate_w).astype(jnp.bfloat16)
    pre_up = dot(x_in, up_w).astype(jnp.bfloat16)
    up_float = pre_up.astype(jnp.float32)
    gelu_val, gelu_vjp = jax.vjp(gelu_tanh, pre_gate.astype(jnp.float32))
    hidden = (gelu_val * up_float).astype(jnp.bfloat16)
    d_hidden = dot(d_out, down_w, ((1,), (1,))).astype(jnp.bfloat16).astype(jnp.float32)
    d_gate = gelu_vjp(d_hidden * up_float)[0].astype(jnp.bfloat16)
    d_up = (d_hidden * gelu_val).astype(jnp.bfloat16)
    return hidden, d_gate, d_up


def solution(mesh):
    row_spec = P(None, AX, None)
    flat_spec = P(None, AX)
    sibling = [(i, i ^ 1) for i in range(128)]

    def shuffle(dtype):
        row = lax.broadcasted_iota(jnp.int32, (HALF, HALF), 0)
        col = lax.broadcasted_iota(jnp.int32, (HALF, HALF), 1)
        return (row == ((col // 8) % 32) * 40 + (col // TILE) * 8 + col % 8).astype(dtype)

    def device_step(x, g, w_gate, w_up, w_down):
        core = lax.axis_index(AX) % 2
        odd = (lax.axis_index(AX) // 2) % 2
        both = jnp.concatenate([w_gate, w_up], axis=0)
        other = lax.ppermute(both, AX, sibling)
        low = jnp.where(core == 0, both, other)
        high = jnp.where(core == 0, other, both)
        chip = jnp.concatenate([low, high], axis=1).reshape(2, 15, HID)
        chip = jnp.where(core == 0, chip[:, :, :HALF], chip[:, :, HALF:])
        chip = dot(jnp.pad(chip, ((0, 0), (0, 1), (0, 0))).reshape(32, HALF), shuffle(jnp.bfloat16)).astype(jnp.bfloat16).reshape(2, 16, HALF)
        spot = lax.axis_index(AX) % 4
        down = jnp.pad(w_down.reshape(20, 2, HALF_WIDTH), ((0, 0), (0, 0), (0, 32))).reshape(20, N, TILE)
        parts = []
        for by in range(N):
            sent = lax.dynamic_index_in_dim(down, (spot + by) % N, 1, keepdims=False)
            parts.append(lax.ppermute(sent, AX, [(64 * c + 4 * k + i, 8 * k + 2 * ((i + by) % N) + c) for c in range(2) for k in range(16) for i in range(N)]))
        parts = jnp.stack(parts)
        spot = (lax.axis_index(AX) // 2) % N
        down = jnp.stack([lax.dynamic_index_in_dim(parts, (spot - i) % N, 0, keepdims=False) for i in range(N)])
        down = down.reshape(2, TILES, 8, TILE).transpose(1, 0, 2, 3).reshape(TILES, 16, TILE)
        x_t = x.transpose(0, 2, 1)
        r_gate, r_up, r_down, _, _, y_t, _ = step_on_chip(x_t, g.transpose(0, 2, 1), chip[0], chip[1], down)
        y = y_t.transpose(0, 2, 1)

        whole = [lax.all_gather(w, AX, axis=1, tiled=True) for w in (w_gate, w_up, w_down)]
        gates, ups, downs = whole[0].reshape(WIDTH, HID), whole[1].reshape(WIDTH, HID), whole[2].reshape(HID, WIDTH)
        d_out = g.reshape(2 * ROWS, WIDTH)
        d_gate, d_up = activations(x.reshape(2 * ROWS, WIDTH), d_out, gates, ups, downs)[1:]
        d_in = (d_out + dot(d_gate, gates, ((1,), (1,))) + dot(d_up, ups, ((1,), (1,)))).astype(jnp.bfloat16)
        del d_in

        both = jnp.concatenate([r_gate, r_up])
        both = lax.dot_general(both, shuffle(jnp.float32), (((1,), (1,)), ((), ())), precision=lax.Precision.HIGHEST, preferred_element_type=jnp.float32)
        both = both.reshape(2, 16, HALF)[:, :15]
        other = lax.ppermute(both, AX, sibling)
        left = jnp.where(core == 0, both, other)
        right = jnp.where(core == 0, other, both)
        chip = jnp.concatenate([left, right], axis=2).reshape(2, 2, 19200)
        mine = jnp.where(core == 0, chip[:, 0], chip[:, 1])
        r_down = r_down[:, :HALF_WIDTH].reshape(2, 20, HALF_WIDTH)
        same = jnp.where(odd == 0, r_down[0], r_down[1])
        cross = jnp.where(odd == 0, r_down[1], r_down[0])
        same = lax.ppermute(same, AX, [(2 * k + c, 64 * c + k) for c in range(2) for k in range(64)])
        cross = lax.ppermute(cross, AX, [(2 * k + c, 64 * c + (k ^ 1)) for c in range(2) for k in range(64)])
        bit = lax.axis_index(AX) % 2
        left = jnp.where(bit == 0, same, cross)
        right = jnp.where(bit == 0, cross, same)
        grad_down = jnp.concatenate([left, right], axis=1).reshape(1, 19200)
        return y, mine[0:1], mine[1:2], grad_down

    return jax.shard_map(device_step, mesh=mesh, in_specs=(row_spec, row_spec, flat_spec, flat_spec, flat_spec), out_specs=(row_spec, flat_spec, flat_spec, flat_spec), check_vma=False)
```

```python
import jax
import jax.numpy as jnp
from jax import lax
from jax.experimental import pallas as pl
from jax.experimental.pallas import tpu as pltpu
from jax.sharding import PartitionSpec as P

AX = "fsdp"
MESH = pl.DeviceIdType.MESH
N = 4
WIDTH = 960
HID = 2560
HALF = 1280
ROWS = 1024
PAD = 1024
SLOPE = 0.7978845608028654
CUBE = 0.044715
TILE = 256
BLOCK = 512
HALF_WIDTH = 480
TILES = 5
WAVES = 10
LEAD = 6
STREAMS = range(3)
WAYS = range(2)
BY_LAST = ((1,), (1,))
CHUNK = ((16, 256), (16, 256), (8, 512))
REDUCE_DIMS = ((0, 1, 2), (1, 2, 0), (2, 0, 1))
GATHER_DIMS = ((2, 1, 0), (1, 0, 2), (0, 2, 1))


def place():
    me = lax.axis_index(AX)
    return (me // 32, (me // 8) % 4, (me // 2) % 4), me % 2


def device(pos, core):
    return (((pos[0] * 4 + pos[1]) * 4 + pos[2]) * 2 + core,)


def shifted(pos, dim, by):
    moved = list(pos)
    moved[dim] = (pos[dim] + by + N) % N
    return tuple(moved)


def greet(pos, core):
    barrier = pltpu.get_barrier_semaphore()
    others = [device(shifted(pos, dim, by), core) for dim in range(3) for by in (1, -1)] + [device(shifted(pos, 2, 2), core), device(pos, 1 - core)]
    for other in others:
        pl.semaphore_signal(barrier, inc=1, device_id=other, device_id_type=MESH)
    pl.semaphore_wait(barrier, len(others))


def step_kernel(x_t, g_t, w_gate, w_up, w_down, out_g, out_u, out_d, h_o, h_s, y_t, y_in, *scratch):
    xv, gv, wg, wu, wd, hv, dav, duv = scratch[:8]
    part = scratch[8:11]
    line = scratch[11:14]
    point = scratch[14:17]
    inbox = [scratch[17 + 6 * s : 23 + 6 * s] for s in STREAMS]
    send_sem, recv_sem, keep_sem, out_sem, back_sem, x_sem, y_send, y_recv, y_load, y_out, xy, y_part, y_other, wt, gather_send, gather_recv, lines, down_v, line_sem = scratch[35:]
    outs = (out_g, out_u, out_d)
    pos, core = place()

    wide = ((x_t, xv, 0), (g_t, gv, 0), (x_t, xv, 1), (g_t, gv, 1))
    weights = (wg, wu, wd)

    def raw(i):
        return pltpu.make_async_copy(wide[i][0].at[wide[i][2]], xy, keep_sem.at[0, i])

    def pair(i):
        buf = wide[i][1].at[wide[i][2]]
        return pltpu.make_async_remote_copy(src_ref=buf.at[pl.ds(0, ROWS)], dst_ref=buf.at[pl.ds(ROWS, ROWS)], send_sem=keep_sem.at[1, i], recv_sem=keep_sem.at[2, i], device_id=device(pos, 1 - core), device_id_type=MESH)

    def widen(i):
        buf, micro = wide[i][1:]
        for lane in range(0, PAD, TILE):
            col = lax.broadcasted_iota(jnp.int32, (WIDTH, TILE), 1) + lane
            row = lax.broadcasted_iota(jnp.int32, (WIDTH, TILE), 0)
            if i % 2 == 0:
                spread = (row == col - (col >> 4)) & ((col & 15) != 15)
            else:
                spread = ((row == col) & (col < HALF_WIDTH)) | ((row == col - 32) & (col >= BLOCK))
            spread = jnp.where(spread, 1.0, 0.0).astype(jnp.bfloat16)
            for t in range(0, ROWS, BLOCK):
                buf[micro, t : t + BLOCK, lane : lane + TILE] = across_rows(xy[:, t : t + BLOCK], spread).astype(jnp.bfloat16)

    def piece(s, n):
        if s == 2:
            return down_v.at[n]
        return (w_gate, w_up)[s].at[:, pl.ds(pl.multiple_of(n * TILE, TILE), TILE)]

    def gather_copy(s, phase, kind, n):
        dims = GATHER_DIMS[s]
        by = 0 if kind < 2 else (-1 if kind == 2 else 1)
        index = list(shifted(pos, dims[phase], by))
        for dim in dims[:phase]:
            index[dim] = slice(None)
        dst = weights[s].at[tuple([n] + index)]
        src = dst
        if kind >= 2:
            lanes = TILE // 2
            dst = dst.at[(slice(None),) * (len(dst.shape) - 1) + (pl.ds((kind - 2) * lanes, lanes),)]
            src = dst
        elif phase == 0:
            src = piece(s, n)
        to = device(shifted(pos, dims[phase], 1 if kind % 2 == 0 else -1), core)
        return pltpu.make_async_remote_copy(src_ref=src, dst_ref=dst, send_sem=gather_send.at[s, phase, kind, n], recv_sem=gather_recv.at[s, phase, kind, n], device_id=to, device_id_type=MESH)

    def gather_step(s, step, n):
        phase = step // 2
        if step % 2 == 1:
            for kind in range(2):
                gather_copy(s, phase, kind, n).wait_recv()
                gather_copy(s, phase, kind + 2, n).start()
            return
        if step > 0:
            for kind in range(2, 4):
                gather_copy(s, phase - 1, kind, n).wait_recv()
        if step < 6:
            for kind in range(2):
                gather_copy(s, phase, kind, n).start()
        else:
            for p in range(3):
                for kind in range(4):
                    gather_copy(s, p, kind, n).wait_send()

    x_loads = [pltpu.make_async_copy(x_t.at[m], xy, x_sem.at[m]) for m in range(2)]
    raw(0).start()
    greet(pos, core)
    spread = []
    for by in range(1, N):
        to = shifted(pos, 2, by)
        quarter = w_down.at[:, pl.ds(pl.multiple_of(to[2] * TILE, TILE), TILE)]
        spread.append(pltpu.make_async_remote_copy(src_ref=quarter, dst_ref=lines.at[pos[2]], send_sem=line_sem.at[0, by], recv_sem=line_sem.at[1, by], device_id=device(to, core), device_id_type=MESH))
        spread[-1].start()
    lines[pos[2]] = w_down[:, pl.ds(pl.multiple_of(pos[2] * TILE, TILE), TILE)]
    row = lax.broadcasted_iota(jnp.int32, (80, 128), 0)
    col = lax.broadcasted_iota(jnp.int32, (80, 128), 1)
    line_row = (row >> 4) * 8 + (row & 7)
    late = jnp.where(line_row >= 20, 1, 0)
    pick = jnp.where(col == ((row >> 3) & 1) * 64 + late * 12 + line_row, 1.0, 0.0).astype(jnp.bfloat16)
    for c in spread:
        c.wait()
    down_v[...] = dot(pick, lines[...].reshape(128, TILE)).astype(jnp.bfloat16).reshape(TILES, 16, TILE)
    for s in STREAMS:
        for n in range(TILES):
            own = down_v[n] if s == 2 else (w_gate, w_up)[s][:, n * TILE : n * TILE + TILE]
            weights[s][n, pos[0], pos[1], pos[2]] = own

    def hidden_out(wave):
        rows = pl.ds(pl.multiple_of((wave // TILES) * ROWS, ROWS), ROWS)
        lanes = pl.ds(pl.multiple_of((wave % TILES) * TILE, TILE), TILE)
        return [pltpu.make_async_copy(hv.at[wave % 2, pl.ds(i * ROWS, ROWS)], dst.at[rows, lanes], out_sem.at[wave % 2, i]) for i, dst in enumerate((h_o, h_s))]

    def half(s, phase, way):
        if phase == 2:
            lanes = CHUNK[s][1] // 2
            return pl.ds(lanes * (1 - way), lanes)
        return pl.ds(2 * (1 - way), 2)

    def send(s, kind, way, wave):
        dims = REDUCE_DIMS[s]
        phase, step = kind // 2, kind % 2
        dim = dims[phase]
        rest = [d for d in range(3) if d not in dims[:phase]]
        buf = (part, line, point)[phase][s].at[wave % 3]
        dest = (pos[dim] + (2 if step == 0 else (1 if way == 0 else 3))) % N
        index = [slice(None)] * len(rest)
        index[rest.index(dim)] = dest
        src = buf.at[tuple(index)]
        if step == 0:
            src = src.at[(slice(None), half(s, phase, way))] if phase == 2 else src.at[half(s, phase, way)]
        to = device(shifted(pos, dim, 1 if way == 0 else -1), core)
        return pltpu.make_async_remote_copy(src_ref=src, dst_ref=inbox[s][kind].at[wave % 4, way], send_sem=send_sem.at[s, kind, way, wave % 4], recv_sem=recv_sem.at[s, kind, way, wave % 4], device_id=to, device_id_type=MESH)

    def activate(wave):
        micro, n = wave // TILES, wave % TILES

        @pl.loop(0, 4)
        def _(i):
            rows = pl.ds(pl.multiple_of(i * BLOCK, BLOCK), BLOCK)
            x_in, d_out = xv[micro, rows, :], gv[micro, rows, :]
            a = dot(x_in, wg[n].reshape(PAD, TILE)).astype(jnp.bfloat16).astype(jnp.float32)
            u = dot(x_in, wu[n].reshape(PAD, TILE)).astype(jnp.bfloat16).astype(jnp.float32)
            dh = sum(dot(d_out[:, q * TILE : q * TILE + TILE], wd[n, :, :, q].reshape(TILE, TILE), BY_LAST) for q in range(N)).astype(jnp.bfloat16).astype(jnp.float32)
            squared = a * a
            t = jnp.tanh(SLOPE * (a + CUBE * (squared * a)))
            cdf = 0.5 * (1.0 + t)
            gelu = a * cdf
            slope = cdf + (0.5 * a) * (1.0 - t * t) * (SLOPE * (1.0 + (3.0 * CUBE) * squared))
            hv[wave % 2, rows, :] = (gelu * u).astype(jnp.bfloat16)
            dav[rows, :] = (dh * u * slope).astype(jnp.bfloat16)
            duv[rows, :] = (dh * gelu).astype(jnp.bfloat16)

    def across_rows(a, b):
        return lax.dot_general(a, b, (((0,), (0,)), ((), ())), preferred_element_type=jnp.float32)

    def products(wave):
        micro = wave // TILES
        for s, d in ((0, dav), (1, duv)):
            for i in range(2):
                r = across_rows(xv[micro, :, i * BLOCK : i * BLOCK + BLOCK], d[...])
                part[s][wave % 3, 2 * i : 2 * i + 2] = r.reshape(2, N, N, 16, TILE)
        for j in range(2):
            r = across_rows(hv[wave % 2], gv[micro, :, j * BLOCK : j * BLOCK + BLOCK]).reshape(N, N, 2, 8, BLOCK)
            for m in range(2):
                part[2][wave % 3, :, :, 2 * m + j] = r[:, :, m]

    def stage(s, step, wave):
        if step > 0:
            kind = step - 1
            phase = kind // 2
            dims = REDUCE_DIMS[s]
            dim = dims[phase]
            rest = [d for d in range(3) if d not in dims[:phase]]
            at = rest.index(dim)
            buf = (part, line, point)[phase][s]
            arrived = inbox[s][kind]
            for way in WAYS:
                send(s, kind, way, wave).wait_recv()
            if kind % 2 == 0:
                for way in WAYS:
                    index = [slice(None)] * len(rest)
                    index[at] = (pos[dim] + (1 if way == 0 else 3)) % N
                    if phase == 2:
                        index += [slice(None), half(s, phase, way)]
                    else:
                        index[[i for i in range(len(rest)) if i != at][0]] = half(s, phase, way)
                    buf[tuple([wave % 3] + index)] += arrived[wave % 4, way]
            else:
                index = [slice(None)] * len(rest)
                index[at] = pos[dim]
                total = buf[tuple([wave % 3] + index)] + arrived[wave % 4, 0] + arrived[wave % 4, 1]
                for way in WAYS:
                    send(s, kind - 1, way, wave).wait_send()
                    send(s, kind, way, wave).wait_send()
                if phase < 2:
                    (line, point)[phase][s][wave % 3] = total
                else:
                    micro, n = wave // TILES, wave % TILES
                    if s < 2:
                        spot = (slice(None), pl.ds(pl.multiple_of(n * TILE, TILE), TILE))
                    else:
                        spot = (pl.ds(pl.multiple_of(n * 8, 8), 8), slice(None))

                    @pl.when(micro == 0)
                    def _():
                        outs[s][spot] = total

                    @pl.when(micro == 1)
                    def _():
                        outs[s][spot] += total
        if step < 6:
            for way in WAYS:
                send(s, step, way, wave).start()

    def hidden_back(m):
        rows = pl.ds(m * ROWS, ROWS)
        return [
            pltpu.make_async_copy(src.at[rows, pl.ds(lane, wide)], dst.at[m, pl.ds(i * ROWS, ROWS), pl.ds(0, wide)], back_sem.at[m, k, i])
            for i, src in enumerate((h_o, h_s))
            for k, (dst, lane, wide) in enumerate(((xv, 0, PAD), (gv, PAD, HALF - PAD)))
        ]

    def y_rows(m, who, i, j):
        rows = slice(who * ROWS + TILE * i, who * ROWS + TILE * i + TILE)
        cols = slice(BLOCK * j, BLOCK * j + HALF_WIDTH)
        return dot(wt[cols, :PAD], xv[m, rows, :], BY_LAST) + dot(wt[cols, PAD:], gv[m, rows, : HALF - PAD], BY_LAST)

    def y_hand(m, i):
        return pltpu.make_async_remote_copy(src_ref=y_part.at[i % 2], dst_ref=y_in.at[m, :, pl.ds(TILE * i, TILE)], send_sem=y_send.at[m, i], recv_sem=y_recv.at[m, i], device_id=device(pos, 1 - core), device_id_type=MESH)

    def y_fetch(m, i):
        return pltpu.make_async_copy(y_in.at[m, :, pl.ds(TILE * i, TILE)], y_other.at[i % 2], y_load.at[m, i])

    def y_done(m, i):
        lanes = pl.ds(TILE * i, TILE)
        return pltpu.make_async_copy(xy.at[:, lanes], y_t.at[m, :, lanes], y_out.at[m, i])

    def y_for_sibling(m, tiles):
        for i in tiles:
            if i >= 2:
                y_hand(m, i - 2).wait_send()
            for j in range(2):
                y_part[i % 2, HALF_WIDTH * j : HALF_WIDTH * j + HALF_WIDTH, :] = y_rows(m, 1, i, j)
            y_hand(m, i).start()

    def y_own(m, tiles):
        for i in tiles:
            if i < 2:
                y_hand(m, i + 2).wait_send()
            y_hand(m, i).wait_recv()
            y_fetch(m, i).start()
        for i in tiles:
            y_fetch(m, i).wait()
            for j in range(2):
                part = slice(HALF_WIDTH * j, HALF_WIDTH * j + HALF_WIDTH)
                lanes = slice(TILE * i, TILE * i + TILE)
                total = y_rows(m, 0, i, j) + y_other[i % 2, part, :]
                xy[part, lanes] = (xy[part, lanes].astype(jnp.float32) + total).astype(jnp.bfloat16)
            y_done(m, i).start()

    @pl.loop(0, LEAD + WAVES + 6)
    def _(turn):
        slot = turn - LEAD

        for step in reversed(range(7)):

            @pl.when((turn >= step) & (turn - step < TILES))
            def _():
                for s in STREAMS:
                    gather_step(s, step, turn - step)

        for m in range(2):
            begin = (LEAD + 1) * m

            @pl.when(turn == begin)
            def _():
                raw(2 * m).wait()
                widen(2 * m)
                raw(2 * m + 1).start()

            @pl.when(turn == begin + 1)
            def _():
                pair(2 * m).start()
                raw(2 * m + 1).wait()
                widen(2 * m + 1)

            @pl.when(turn == begin + 2)
            def _():
                pair(2 * m + 1).start()
                (x_loads[0] if m else raw(2)).start()

        for micro in range(2):

            @pl.when(slot == micro * TILES)
            def _():
                for i in range(2):
                    pair(2 * micro + i).wait()

        @pl.when((slot >= 2) & (slot < WAVES + 1))
        def _():
            for c in hidden_out(slot - 2):
                c.wait()

        @pl.when((slot >= 0) & (slot < WAVES))
        def _():
            activate(slot)
            products(slot)
            for c in hidden_out(slot):
                c.start()

        for step in range(7):

            @pl.when((slot >= step) & (slot - step < WAVES))
            def _():
                for s in STREAMS:
                    stage(s, step, slot - step)

        @pl.when(slot == 6)
        def _():
            for c in hidden_back(0):
                c.start()
            for i in range(TILES):
                for q in range(N):
                    wt[q * TILE : q * TILE + TILE, i * TILE : i * TILE + TILE] = wd[i, :, :, q].reshape(TILE, TILE).T

        @pl.when(slot == 7)
        def _():
            for c in hidden_back(0):
                c.wait()

        @pl.when(slot == WAVES)
        def _():
            for c in hidden_out(WAVES - 1):
                c.wait()
            for c in hidden_back(1):
                c.start()

        @pl.when(slot == 11)
        def _():
            for i in range(4):
                y_done(0, i).wait()
            x_loads[1].start()
            for c in hidden_back(1):
                c.wait()

        for m in range(2):
            for t in range(2):

                @pl.when(slot == 7 + 4 * m + t)
                def _():
                    y_for_sibling(m, range(2 * t, 2 * t + 2))

                @pl.when(slot == 9 + 4 * m + t)
                def _():
                    if t == 0:
                        x_loads[m].wait()
                    y_own(m, range(2 * t, 2 * t + 2))

    for i in range(4):
        y_done(1, i).wait()


def step_on_chip(*operands):
    hbm = pl.BlockSpec(memory_space=pl.ANY)
    vmem = pl.BlockSpec(memory_space=pltpu.VMEM)
    f32 = jnp.float32
    bf16 = jnp.bfloat16
    scratch = [pltpu.VMEM((2, 2 * ROWS, PAD), bf16)] * 2
    scratch += [pltpu.VMEM((TILES, N, N, N, 16, TILE), bf16)] * 3
    scratch += [pltpu.VMEM((2, 2 * ROWS, TILE), bf16)] + [pltpu.VMEM((2 * ROWS, TILE), bf16)] * 2
    scratch += [pltpu.VMEM((3, N, N, N) + CHUNK[s], f32) for s in STREAMS]
    scratch += [pltpu.VMEM((3, N, N) + CHUNK[s], f32) for s in STREAMS]
    scratch += [pltpu.VMEM((3, N) + CHUNK[s], f32) for s in STREAMS]
    for s in STREAMS:
        rows, lanes = CHUNK[s]
        scratch += [pltpu.VMEM((4, 2) + lead + CHUNK[s], f32) for lead in ((2, N), (N, N), (2,), (N,))]
        scratch += [pltpu.VMEM((4, 2, rows, lanes // 2), f32), pltpu.VMEM((4, 2) + CHUNK[s], f32)]
    scratch += [pltpu.SemaphoreType.DMA((3, 6, 2, 4)), pltpu.SemaphoreType.DMA((3, 6, 2, 4)), pltpu.SemaphoreType.DMA((3, 4)), pltpu.SemaphoreType.DMA((2, 2))]
    scratch += [pltpu.SemaphoreType.DMA((2, 2, 2)), pltpu.SemaphoreType.DMA((2,))] + [pltpu.SemaphoreType.DMA((2, 4))] * 4
    scratch += [pltpu.VMEM((WIDTH, ROWS), bf16), pltpu.VMEM((2, WIDTH, TILE), f32), pltpu.VMEM((2, WIDTH, TILE), f32), pltpu.VMEM((PAD, HALF), bf16), pltpu.SemaphoreType.DMA((3, 3, 4, TILES)), pltpu.SemaphoreType.DMA((3, 3, 4, TILES)), pltpu.VMEM((N, 32, TILE), bf16), pltpu.VMEM((TILES, 16, TILE), bf16), pltpu.SemaphoreType.DMA((2, N))]
    return pl.pallas_call(
        step_kernel,
        out_shape=[jax.ShapeDtypeStruct((16, HALF), f32), jax.ShapeDtypeStruct((16, HALF), f32), jax.ShapeDtypeStruct((40, BLOCK), f32)] + [jax.ShapeDtypeStruct((2 * ROWS, HALF), bf16)] * 2 + [jax.ShapeDtypeStruct((2, WIDTH, ROWS), bf16), jax.ShapeDtypeStruct((2, WIDTH, ROWS), f32)],
        in_specs=[hbm] * 2 + [vmem] * 3,
        out_specs=[vmem] * 3 + [hbm] * 4,
        scratch_shapes=scratch,
        compiler_params=pltpu.CompilerParams(collective_id=0, has_side_effects=True, vmem_limit_bytes=63 * 2**20),
        name="mlp_step",
    )(*operands)


def gelu_tanh(z):
    return jax.nn.gelu(z, approximate=True)


def dot(a, b, dims=((1,), (0,))):
    return lax.dot_general(a, b, (dims, ((), ())), preferred_element_type=jnp.float32)


def activations(x_in, d_out, gate_w, up_w, down_w):
    pre_gate = dot(x_in, gate_w).astype(jnp.bfloat16)
    pre_up = dot(x_in, up_w).astype(jnp.bfloat16)
    up_float = pre_up.astype(jnp.float32)
    gelu_val, gelu_vjp = jax.vjp(gelu_tanh, pre_gate.astype(jnp.float32))
    hidden = (gelu_val * up_float).astype(jnp.bfloat16)
    d_hidden = dot(d_out, down_w, BY_LAST).astype(jnp.bfloat16).astype(jnp.float32)
    d_gate = gelu_vjp(d_hidden * up_float)[0].astype(jnp.bfloat16)
    d_up = (d_hidden * gelu_val).astype(jnp.bfloat16)
    return hidden, d_gate, d_up


def solution(mesh):
    row_spec = P(None, AX, None)
    flat_spec = P(None, AX)
    sibling = [(i, i ^ 1) for i in range(128)]

    def shuffle(dtype):
        row = lax.broadcasted_iota(jnp.int32, (HALF, HALF), 0)
        col = lax.broadcasted_iota(jnp.int32, (HALF, HALF), 1)
        return (row == ((col // 8) % 32) * 40 + (col // TILE) * 8 + col % 8).astype(dtype)

    def device_step(x, g, w_gate, w_up, w_down):
        core = lax.axis_index(AX) % 2
        odd = (lax.axis_index(AX) // 2) % 2
        both = jnp.concatenate([w_gate, w_up], axis=0)
        other = lax.ppermute(both, AX, sibling)
        low = jnp.where(core == 0, both, other)
        high = jnp.where(core == 0, other, both)
        chip = jnp.concatenate([low, high], axis=1).reshape(2, 15, HID)
        chip = jnp.where(core == 0, chip[:, :, :HALF], chip[:, :, HALF:])
        chip = dot(jnp.pad(chip, ((0, 0), (0, 1), (0, 0))).reshape(32, HALF), shuffle(jnp.bfloat16)).astype(jnp.bfloat16).reshape(2, 16, HALF)
        down = lax.ppermute(w_down, AX, [(64 * c + k, 2 * k + c) for c in range(2) for k in range(64)])
        down = jnp.pad(down.reshape(20, 2, HALF_WIDTH), ((0, 12), (0, 0), (0, 32))).reshape(32, PAD)
        x_t = x.transpose(0, 2, 1)
        r_gate, r_up, r_down, _, _, y_t, _ = step_on_chip(x_t, g.transpose(0, 2, 1), chip[0], chip[1], down)
        y = y_t.transpose(0, 2, 1)

        whole = [lax.all_gather(w, AX, axis=1, tiled=True) for w in (w_gate, w_up, w_down)]
        gates, ups, downs = whole[0].reshape(WIDTH, HID), whole[1].reshape(WIDTH, HID), whole[2].reshape(HID, WIDTH)
        d_out = g.reshape(2 * ROWS, WIDTH)
        d_gate, d_up = activations(x.reshape(2 * ROWS, WIDTH), d_out, gates, ups, downs)[1:]
        d_in = (d_out + dot(d_gate, gates, BY_LAST) + dot(d_up, ups, BY_LAST)).astype(jnp.bfloat16)
        del d_in

        both = jnp.concatenate([r_gate, r_up])
        high = both.astype(jnp.bfloat16)
        rest = both - high.astype(jnp.float32)
        mid = rest.astype(jnp.bfloat16)
        low = (rest - mid.astype(jnp.float32)).astype(jnp.bfloat16)
        both = dot(jnp.concatenate([high, mid, low]), shuffle(jnp.bfloat16), BY_LAST).reshape(3, 32, HALF)
        both = (both[0] + both[1]) + both[2]
        both = both.reshape(2, 16, HALF)[:, :15]
        other = lax.ppermute(both, AX, sibling)
        left = jnp.where(core == 0, both, other)
        right = jnp.where(core == 0, other, both)
        chip = jnp.concatenate([left, right], axis=2).reshape(2, 2, 19200)
        mine = jnp.where(core == 0, chip[:, 0], chip[:, 1])
        r_down = r_down[:, :HALF_WIDTH].reshape(2, 20, HALF_WIDTH)
        same = jnp.where(odd == 0, r_down[0], r_down[1])
        cross = jnp.where(odd == 0, r_down[1], r_down[0])
        same = lax.ppermute(same, AX, [(2 * k + c, 64 * c + k) for c in range(2) for k in range(64)])
        cross = lax.ppermute(cross, AX, [(2 * k + c, 64 * c + (k ^ 1)) for c in range(2) for k in range(64)])
        bit = lax.axis_index(AX) % 2
        left = jnp.where(bit == 0, same, cross)
        right = jnp.where(bit == 0, cross, same)
        grad_down = jnp.concatenate([left, right], axis=1).reshape(1, 19200)
        return y, mine[0:1], mine[1:2], grad_down

    return jax.shard_map(device_step, mesh=mesh, in_specs=(row_spec, row_spec, flat_spec, flat_spec, flat_spec), out_specs=(row_spec, flat_spec, flat_spec, flat_spec), check_vma=False)
```

```python
import jax
import jax.numpy as jnp
from jax import lax
from jax.experimental import pallas as pl
from jax.experimental.pallas import tpu as pltpu
from jax.sharding import PartitionSpec as P

AX = "fsdp"
MESH = pl.DeviceIdType.MESH
N = 4
WIDTH = 960
HID = 2560
HALF = 1280
ROWS = 1024
PAD = 1024
SLOPE = 0.7978845608028654
CUBE = 0.044715
TILE = 256
BLOCK = 512
HALF_WIDTH = 480
TILES = 5
WAVES = 10
LEAD = 6
STREAMS = range(3)
WAYS = range(2)
BY_LAST = ((1,), (1,))
CHUNK = ((16, 256), (16, 256), (8, 512))
REDUCE_DIMS = ((0, 1, 2), (1, 2, 0), (2, 0, 1))
GATHER_DIMS = ((2, 1, 0), (1, 0, 2), (0, 2, 1))


def place():
    me = lax.axis_index(AX)
    return (me // 32, (me // 8) % 4, (me // 2) % 4), me % 2


def device(pos, core):
    return (((pos[0] * 4 + pos[1]) * 4 + pos[2]) * 2 + core,)


def shifted(pos, dim, by):
    moved = list(pos)
    moved[dim] = (pos[dim] + by + N) % N
    return tuple(moved)


def greet(pos, core):
    barrier = pltpu.get_barrier_semaphore()
    others = [device(shifted(pos, dim, by), core) for dim in range(3) for by in (1, -1)] + [device(shifted(pos, 2, 2), core), device(pos, 1 - core)]
    for other in others:
        pl.semaphore_signal(barrier, inc=1, device_id=other, device_id_type=MESH)
    pl.semaphore_wait(barrier, len(others))


def step_kernel(x_t, g_t, w_gate, w_up, w_down, out_g, out_u, out_d, h_o, h_s, y_t, y_in, *scratch):
    xv, gv, wg, wu, wd, hv, dav, duv = scratch[:8]
    part = scratch[8:11]
    line = scratch[11:14]
    point = scratch[14:17]
    inbox = [scratch[17 + 6 * s : 23 + 6 * s] for s in STREAMS]
    send_sem, recv_sem, keep_sem, out_sem, back_sem, x_sem, y_send, y_recv, y_load, y_out, xy, y_part, y_other, wt, gather_send, gather_recv, lines, down_v, line_sem = scratch[35:]
    outs = (out_g, out_u, out_d)
    pos, core = place()

    wide = ((x_t, xv, 0), (g_t, gv, 0), (x_t, xv, 1), (g_t, gv, 1))
    weights = (wg, wu, wd)

    def raw(i):
        return pltpu.make_async_copy(wide[i][0].at[wide[i][2]], xy, keep_sem.at[0, i])

    def pair(i):
        buf = wide[i][1].at[wide[i][2]]
        return pltpu.make_async_remote_copy(src_ref=buf.at[pl.ds(0, ROWS)], dst_ref=buf.at[pl.ds(ROWS, ROWS)], send_sem=keep_sem.at[1, i], recv_sem=keep_sem.at[2, i], device_id=device(pos, 1 - core), device_id_type=MESH)

    def widen(i, start):
        buf, micro = wide[i][1:]
        for lane in range(start, start + BLOCK, TILE):
            col = lax.broadcasted_iota(jnp.int32, (WIDTH, TILE), 1) + lane
            row = lax.broadcasted_iota(jnp.int32, (WIDTH, TILE), 0)
            if i % 2 == 0:
                spread = (row == col - (col >> 4)) & ((col & 15) != 15)
            else:
                spread = ((row == col) & (col < HALF_WIDTH)) | ((row == col - 32) & (col >= BLOCK))
            spread = jnp.where(spread, 1.0, 0.0).astype(jnp.bfloat16)
            for t in range(0, ROWS, BLOCK):
                buf[micro, t : t + BLOCK, lane : lane + TILE] = across_rows(xy[:, t : t + BLOCK], spread).astype(jnp.bfloat16)

    def piece(s, n):
        if s == 2:
            return down_v.at[n]
        return (w_gate, w_up)[s].at[:, pl.ds(pl.multiple_of(n * TILE, TILE), TILE)]

    def gather_copy(s, phase, kind, n):
        dims = GATHER_DIMS[s]
        by = 0 if kind < 2 else (-1 if kind == 2 else 1)
        index = list(shifted(pos, dims[phase], by))
        for dim in dims[:phase]:
            index[dim] = slice(None)
        dst = weights[s].at[tuple([n] + index)]
        src = dst
        if kind >= 2:
            lanes = TILE // 2
            dst = dst.at[(slice(None),) * (len(dst.shape) - 1) + (pl.ds((kind - 2) * lanes, lanes),)]
            src = dst
        elif phase == 0:
            src = piece(s, n)
        to = device(shifted(pos, dims[phase], 1 if kind % 2 == 0 else -1), core)
        return pltpu.make_async_remote_copy(src_ref=src, dst_ref=dst, send_sem=gather_send.at[s, phase, kind, n], recv_sem=gather_recv.at[s, phase, kind, n], device_id=to, device_id_type=MESH)

    def gather_step(s, step, n):
        phase = step // 2
        if step % 2 == 1:
            for kind in range(2):
                gather_copy(s, phase, kind, n).wait_recv()
                gather_copy(s, phase, kind + 2, n).start()
            return
        if step > 0:
            for kind in range(2, 4):
                gather_copy(s, phase - 1, kind, n).wait_recv()
        if step < 6:
            for kind in range(2):
                gather_copy(s, phase, kind, n).start()
        else:
            for p in range(3):
                for kind in range(4):
                    gather_copy(s, p, kind, n).wait_send()

    x_loads = [pltpu.make_async_copy(x_t.at[m], xy, x_sem.at[m]) for m in range(2)]
    raw(0).start()
    greet(pos, core)
    spread = []
    for by in range(1, N):
        to = shifted(pos, 2, by)
        quarter = w_down.at[:, pl.ds(pl.multiple_of(to[2] * TILE, TILE), TILE)]
        spread.append(pltpu.make_async_remote_copy(src_ref=quarter, dst_ref=lines.at[pos[2]], send_sem=line_sem.at[0, by], recv_sem=line_sem.at[1, by], device_id=device(to, core), device_id_type=MESH))
        spread[-1].start()
    lines[pos[2]] = w_down[:, pl.ds(pl.multiple_of(pos[2] * TILE, TILE), TILE)]
    row = lax.broadcasted_iota(jnp.int32, (80, 128), 0)
    col = lax.broadcasted_iota(jnp.int32, (80, 128), 1)
    line_row = (row >> 4) * 8 + (row & 7)
    late = jnp.where(line_row >= 20, 1, 0)
    pick = jnp.where(col == ((row >> 3) & 1) * 64 + late * 12 + line_row, 1.0, 0.0).astype(jnp.bfloat16)
    for c in spread:
        c.wait()
    down_v[...] = dot(pick, lines[...].reshape(128, TILE)).astype(jnp.bfloat16).reshape(TILES, 16, TILE)
    for s in STREAMS:
        for n in range(TILES):
            own = down_v[n] if s == 2 else (w_gate, w_up)[s][:, n * TILE : n * TILE + TILE]
            weights[s][n, pos[0], pos[1], pos[2]] = own

    def hidden_out(wave):
        rows = pl.ds(pl.multiple_of((wave // TILES) * ROWS, ROWS), ROWS)
        lanes = pl.ds(pl.multiple_of((wave % TILES) * TILE, TILE), TILE)
        return [pltpu.make_async_copy(hv.at[wave % 2, pl.ds(i * ROWS, ROWS)], dst.at[rows, lanes], out_sem.at[wave % 2, i]) for i, dst in enumerate((h_o, h_s))]

    def half(s, phase, way):
        if phase == 2:
            lanes = CHUNK[s][1] // 2
            return pl.ds(lanes * (1 - way), lanes)
        return pl.ds(2 * (1 - way), 2)

    def send(s, kind, way, wave):
        dims = REDUCE_DIMS[s]
        phase, step = kind // 2, kind % 2
        dim = dims[phase]
        rest = [d for d in range(3) if d not in dims[:phase]]
        buf = (part, line, point)[phase][s].at[wave % 3]
        dest = (pos[dim] + (2 if step == 0 else (1 if way == 0 else 3))) % N
        index = [slice(None)] * len(rest)
        index[rest.index(dim)] = dest
        src = buf.at[tuple(index)]
        if step == 0:
            src = src.at[(slice(None), half(s, phase, way))] if phase == 2 else src.at[half(s, phase, way)]
        to = device(shifted(pos, dim, 1 if way == 0 else -1), core)
        return pltpu.make_async_remote_copy(src_ref=src, dst_ref=inbox[s][kind].at[wave % 4, way], send_sem=send_sem.at[s, kind, way, wave % 4], recv_sem=recv_sem.at[s, kind, way, wave % 4], device_id=to, device_id_type=MESH)

    def activate(wave):
        micro, n = wave // TILES, wave % TILES

        @pl.loop(0, 4)
        def _(i):
            rows = pl.ds(pl.multiple_of(i * BLOCK, BLOCK), BLOCK)
            x_in, d_out = xv[micro, rows, :], gv[micro, rows, :]
            a = dot(x_in, wg[n].reshape(PAD, TILE)).astype(jnp.bfloat16).astype(jnp.float32)
            u = dot(x_in, wu[n].reshape(PAD, TILE)).astype(jnp.bfloat16).astype(jnp.float32)
            dh = sum(dot(d_out[:, q * TILE : q * TILE + TILE], wd[n, :, :, q].reshape(TILE, TILE), BY_LAST) for q in range(N)).astype(jnp.bfloat16).astype(jnp.float32)
            squared = a * a
            t = jnp.tanh(SLOPE * (a + CUBE * (squared * a)))
            cdf = 0.5 * (1.0 + t)
            gelu = a * cdf
            slope = cdf + (0.5 * a) * (1.0 - t * t) * (SLOPE * (1.0 + (3.0 * CUBE) * squared))
            hv[wave % 2, rows, :] = (gelu * u).astype(jnp.bfloat16)
            dav[rows, :] = (dh * u * slope).astype(jnp.bfloat16)
            duv[rows, :] = (dh * gelu).astype(jnp.bfloat16)

    def across_rows(a, b):
        return lax.dot_general(a, b, (((0,), (0,)), ((), ())), preferred_element_type=jnp.float32)

    def products(wave):
        micro = wave // TILES
        for s, d in ((0, dav), (1, duv)):
            for i in range(2):
                r = across_rows(xv[micro, :, i * BLOCK : i * BLOCK + BLOCK], d[...])
                part[s][wave % 3, 2 * i : 2 * i + 2] = r.reshape(2, N, N, 16, TILE)
        for j in range(2):
            r = across_rows(hv[wave % 2], gv[micro, :, j * BLOCK : j * BLOCK + BLOCK]).reshape(N, N, 2, 8, BLOCK)
            for m in range(2):
                part[2][wave % 3, :, :, 2 * m + j] = r[:, :, m]

    def stage(s, step, wave):
        if step > 0:
            kind = step - 1
            phase = kind // 2
            dims = REDUCE_DIMS[s]
            dim = dims[phase]
            rest = [d for d in range(3) if d not in dims[:phase]]
            at = rest.index(dim)
            buf = (part, line, point)[phase][s]
            arrived = inbox[s][kind]
            for way in WAYS:
                send(s, kind, way, wave).wait_recv()
            if kind % 2 == 0:
                for way in WAYS:
                    index = [slice(None)] * len(rest)
                    index[at] = (pos[dim] + (1 if way == 0 else 3)) % N
                    if phase == 2:
                        index += [slice(None), half(s, phase, way)]
                    else:
                        index[[i for i in range(len(rest)) if i != at][0]] = half(s, phase, way)
                    buf[tuple([wave % 3] + index)] += arrived[wave % 4, way]
            else:
                index = [slice(None)] * len(rest)
                index[at] = pos[dim]
                total = buf[tuple([wave % 3] + index)] + arrived[wave % 4, 0] + arrived[wave % 4, 1]
                for way in WAYS:
                    send(s, kind - 1, way, wave).wait_send()
                    send(s, kind, way, wave).wait_send()
                if phase < 2:
                    (line, point)[phase][s][wave % 3] = total
                else:
                    micro, n = wave // TILES, wave % TILES
                    if s < 2:
                        spot = (slice(None), pl.ds(pl.multiple_of(n * TILE, TILE), TILE))
                    else:
                        spot = (pl.ds(pl.multiple_of(n * 8, 8), 8), slice(None))

                    @pl.when(micro == 0)
                    def _():
                        outs[s][spot] = total

                    @pl.when(micro == 1)
                    def _():
                        outs[s][spot] += total
        if step < 6:
            for way in WAYS:
                send(s, step, way, wave).start()

    def hidden_back(m):
        rows = pl.ds(m * ROWS, ROWS)
        return [
            pltpu.make_async_copy(src.at[rows, pl.ds(lane, wide)], dst.at[m, pl.ds(i * ROWS, ROWS), pl.ds(0, wide)], back_sem.at[m, k, i])
            for i, src in enumerate((h_o, h_s))
            for k, (dst, lane, wide) in enumerate(((xv, 0, PAD), (gv, PAD, HALF - PAD)))
        ]

    def y_rows(m, who, i, j):
        rows = slice(who * ROWS + TILE * i, who * ROWS + TILE * i + TILE)
        cols = slice(BLOCK * j, BLOCK * j + HALF_WIDTH)
        return dot(wt[cols, :PAD], xv[m, rows, :], BY_LAST) + dot(wt[cols, PAD:], gv[m, rows, : HALF - PAD], BY_LAST)

    def y_hand(m, i):
        return pltpu.make_async_remote_copy(src_ref=y_part.at[i % 2], dst_ref=y_in.at[m, :, pl.ds(TILE * i, TILE)], send_sem=y_send.at[m, i], recv_sem=y_recv.at[m, i], device_id=device(pos, 1 - core), device_id_type=MESH)

    def y_fetch(m, i):
        return pltpu.make_async_copy(y_in.at[m, :, pl.ds(TILE * i, TILE)], y_other.at[i % 2], y_load.at[m, i])

    def y_done(m, i):
        lanes = pl.ds(TILE * i, TILE)
        return pltpu.make_async_copy(xy.at[:, lanes], y_t.at[m, :, lanes], y_out.at[m, i])

    def y_for_sibling(m, tiles):
        for i in tiles:
            if i >= 2:
                y_hand(m, i - 2).wait_send()
            for j in range(2):
                y_part[i % 2, HALF_WIDTH * j : HALF_WIDTH * j + HALF_WIDTH, :] = y_rows(m, 1, i, j)
            y_hand(m, i).start()

    def y_own(m, tiles):
        for i in tiles:
            if i < 2:
                y_hand(m, i + 2).wait_send()
            y_hand(m, i).wait_recv()
            y_fetch(m, i).start()
        for i in tiles:
            y_fetch(m, i).wait()
            for j in range(2):
                part = slice(HALF_WIDTH * j, HALF_WIDTH * j + HALF_WIDTH)
                lanes = slice(TILE * i, TILE * i + TILE)
                total = y_rows(m, 0, i, j) + y_other[i % 2, part, :]
                xy[part, lanes] = (xy[part, lanes].astype(jnp.float32) + total).astype(jnp.bfloat16)
            y_done(m, i).start()

    @pl.loop(0, LEAD + WAVES + 6)
    def _(turn):
        slot = turn - LEAD

        for step in reversed(range(7)):

            @pl.when((turn >= step) & (turn - step < TILES))
            def _():
                for s in STREAMS:
                    gather_step(s, step, turn - step)

        for m in range(2):
            for i in range(2):
                begin = LEAD * m + 2 * i

                @pl.when(turn == begin)
                def _():
                    if i:
                        pair(2 * m).start()
                    raw(2 * m + i).wait()
                    widen(2 * m + i, 0)

                @pl.when(turn == begin + 1)
                def _():
                    widen(2 * m + i, BLOCK)
                    (x_loads[0] if m and i else raw(2 * m + i + 1)).start()

            @pl.when(turn == LEAD * m + 4)
            def _():
                pair(2 * m + 1).start()

        for micro in range(2):

            @pl.when(slot == micro * TILES)
            def _():
                for i in range(2):
                    pair(2 * micro + i).wait()

        @pl.when((slot >= 2) & (slot < WAVES + 1))
        def _():
            for c in hidden_out(slot - 2):
                c.wait()

        @pl.when((slot >= 0) & (slot < WAVES))
        def _():
            activate(slot)
            products(slot)
            for c in hidden_out(slot):
                c.start()

        for step in range(7):

            @pl.when((slot >= step) & (slot - step < WAVES))
            def _():
                for s in STREAMS:
                    stage(s, step, slot - step)

        @pl.when(slot == 6)
        def _():
            for c in hidden_back(0):
                c.start()
            for i in range(TILES):
                for q in range(N):
                    wt[q * TILE : q * TILE + TILE, i * TILE : i * TILE + TILE] = wd[i, :, :, q].reshape(TILE, TILE).T

        @pl.when(slot == 7)
        def _():
            for c in hidden_back(0):
                c.wait()

        @pl.when(slot == WAVES)
        def _():
            for c in hidden_out(WAVES - 1):
                c.wait()
            for c in hidden_back(1):
                c.start()

        @pl.when(slot == 11)
        def _():
            for i in range(4):
                y_done(0, i).wait()
            x_loads[1].start()
            for c in hidden_back(1):
                c.wait()

        for m in range(2):
            for t in range(2):

                @pl.when(slot == 7 + 4 * m + t)
                def _():
                    y_for_sibling(m, range(2 * t, 2 * t + 2))

                @pl.when(slot == 9 + 4 * m + t)
                def _():
                    if t == 0:
                        x_loads[m].wait()
                    y_own(m, range(2 * t, 2 * t + 2))

    for i in range(4):
        y_done(1, i).wait()


def step_on_chip(*operands):
    hbm = pl.BlockSpec(memory_space=pl.ANY)
    vmem = pl.BlockSpec(memory_space=pltpu.VMEM)
    f32 = jnp.float32
    bf16 = jnp.bfloat16
    scratch = [pltpu.VMEM((2, 2 * ROWS, PAD), bf16)] * 2
    scratch += [pltpu.VMEM((TILES, N, N, N, 16, TILE), bf16)] * 3
    scratch += [pltpu.VMEM((2, 2 * ROWS, TILE), bf16)] + [pltpu.VMEM((2 * ROWS, TILE), bf16)] * 2
    scratch += [pltpu.VMEM((3, N, N, N) + CHUNK[s], f32) for s in STREAMS]
    scratch += [pltpu.VMEM((3, N, N) + CHUNK[s], f32) for s in STREAMS]
    scratch += [pltpu.VMEM((3, N) + CHUNK[s], f32) for s in STREAMS]
    for s in STREAMS:
        rows, lanes = CHUNK[s]
        scratch += [pltpu.VMEM((4, 2) + lead + CHUNK[s], f32) for lead in ((2, N), (N, N), (2,), (N,))]
        scratch += [pltpu.VMEM((4, 2, rows, lanes // 2), f32), pltpu.VMEM((4, 2) + CHUNK[s], f32)]
    scratch += [pltpu.SemaphoreType.DMA((3, 6, 2, 4)), pltpu.SemaphoreType.DMA((3, 6, 2, 4)), pltpu.SemaphoreType.DMA((3, 4)), pltpu.SemaphoreType.DMA((2, 2))]
    scratch += [pltpu.SemaphoreType.DMA((2, 2, 2)), pltpu.SemaphoreType.DMA((2,))] + [pltpu.SemaphoreType.DMA((2, 4))] * 4
    scratch += [pltpu.VMEM((WIDTH, ROWS), bf16), pltpu.VMEM((2, WIDTH, TILE), f32), pltpu.VMEM((2, WIDTH, TILE), f32), pltpu.VMEM((PAD, HALF), bf16), pltpu.SemaphoreType.DMA((3, 3, 4, TILES)), pltpu.SemaphoreType.DMA((3, 3, 4, TILES)), pltpu.VMEM((N, 32, TILE), bf16), pltpu.VMEM((TILES, 16, TILE), bf16), pltpu.SemaphoreType.DMA((2, N))]
    return pl.pallas_call(
        step_kernel,
        out_shape=[jax.ShapeDtypeStruct((16, HALF), f32), jax.ShapeDtypeStruct((16, HALF), f32), jax.ShapeDtypeStruct((40, BLOCK), f32)] + [jax.ShapeDtypeStruct((2 * ROWS, HALF), bf16)] * 2 + [jax.ShapeDtypeStruct((2, WIDTH, ROWS), bf16), jax.ShapeDtypeStruct((2, WIDTH, ROWS), f32)],
        in_specs=[hbm] * 2 + [vmem] * 3,
        out_specs=[vmem] * 3 + [hbm] * 4,
        scratch_shapes=scratch,
        compiler_params=pltpu.CompilerParams(collective_id=0, has_side_effects=True, vmem_limit_bytes=63 * 2**20),
        name="mlp_step",
    )(*operands)


def gelu_tanh(z):
    return jax.nn.gelu(z, approximate=True)


def dot(a, b, dims=((1,), (0,))):
    return lax.dot_general(a, b, (dims, ((), ())), preferred_element_type=jnp.float32)


def activations(x_in, d_out, gate_w, up_w, down_w):
    pre_gate = dot(x_in, gate_w).astype(jnp.bfloat16)
    pre_up = dot(x_in, up_w).astype(jnp.bfloat16)
    up_float = pre_up.astype(jnp.float32)
    gelu_val, gelu_vjp = jax.vjp(gelu_tanh, pre_gate.astype(jnp.float32))
    hidden = (gelu_val * up_float).astype(jnp.bfloat16)
    d_hidden = dot(d_out, down_w, BY_LAST).astype(jnp.bfloat16).astype(jnp.float32)
    d_gate = gelu_vjp(d_hidden * up_float)[0].astype(jnp.bfloat16)
    d_up = (d_hidden * gelu_val).astype(jnp.bfloat16)
    return hidden, d_gate, d_up


def solution(mesh):
    row_spec = P(None, AX, None)
    flat_spec = P(None, AX)
    sibling = [(i, i ^ 1) for i in range(128)]

    def shuffle(dtype):
        row = lax.broadcasted_iota(jnp.int32, (HALF, HALF), 0)
        col = lax.broadcasted_iota(jnp.int32, (HALF, HALF), 1)
        return (row == ((col // 8) % 32) * 40 + (col // TILE) * 8 + col % 8).astype(dtype)

    def device_step(x, g, w_gate, w_up, w_down):
        core = lax.axis_index(AX) % 2
        odd = (lax.axis_index(AX) // 2) % 2
        both = jnp.concatenate([w_gate, w_up], axis=0)
        other = lax.ppermute(both, AX, sibling)
        low = jnp.where(core == 0, both, other)
        high = jnp.where(core == 0, other, both)
        chip = jnp.concatenate([low, high], axis=1).reshape(2, 15, HID)
        chip = jnp.where(core == 0, chip[:, :, :HALF], chip[:, :, HALF:])
        chip = dot(jnp.pad(chip, ((0, 0), (0, 1), (0, 0))).reshape(32, HALF), shuffle(jnp.bfloat16)).astype(jnp.bfloat16).reshape(2, 16, HALF)
        down = lax.ppermute(w_down, AX, [(64 * c + k, 2 * k + c) for c in range(2) for k in range(64)])
        down = jnp.pad(down.reshape(20, 2, HALF_WIDTH), ((0, 12), (0, 0), (0, 32))).reshape(32, PAD)
        x_t = x.transpose(0, 2, 1)
        r_gate, r_up, r_down, _, _, y_t, _ = step_on_chip(x_t, g.transpose(0, 2, 1), chip[0], chip[1], down)
        y = y_t.transpose(0, 2, 1)

        whole = [lax.all_gather(w, AX, axis=1, tiled=True) for w in (w_gate, w_up, w_down)]
        gates, ups, downs = whole[0].reshape(WIDTH, HID), whole[1].reshape(WIDTH, HID), whole[2].reshape(HID, WIDTH)
        d_out = g.reshape(2 * ROWS, WIDTH)
        d_gate, d_up = activations(x.reshape(2 * ROWS, WIDTH), d_out, gates, ups, downs)[1:]
        d_in = (d_out + dot(d_gate, gates, BY_LAST) + dot(d_up, ups, BY_LAST)).astype(jnp.bfloat16)
        del d_in

        both = jnp.concatenate([r_gate, r_up])
        high = both.astype(jnp.bfloat16)
        rest = both - high.astype(jnp.float32)
        mid = rest.astype(jnp.bfloat16)
        low = (rest - mid.astype(jnp.float32)).astype(jnp.bfloat16)
        both = dot(jnp.concatenate([high, mid, low]), shuffle(jnp.bfloat16), BY_LAST).reshape(3, 32, HALF)
        both = (both[0] + both[1]) + both[2]
        both = both.reshape(2, 16, HALF)[:, :15]
        other = lax.ppermute(both, AX, sibling)
        left = jnp.where(core == 0, both, other)
        right = jnp.where(core == 0, other, both)
        chip = jnp.concatenate([left, right], axis=2).reshape(2, 2, 19200)
        mine = jnp.where(core == 0, chip[:, 0], chip[:, 1])
        r_down = r_down[:, :HALF_WIDTH].reshape(2, 20, HALF_WIDTH)
        same = jnp.where(odd == 0, r_down[0], r_down[1])
        cross = jnp.where(odd == 0, r_down[1], r_down[0])
        same = lax.ppermute(same, AX, [(2 * k + c, 64 * c + k) for c in range(2) for k in range(64)])
        cross = lax.ppermute(cross, AX, [(2 * k + c, 64 * c + (k ^ 1)) for c in range(2) for k in range(64)])
        bit = lax.axis_index(AX) % 2
        left = jnp.where(bit == 0, same, cross)
        right = jnp.where(bit == 0, cross, same)
        grad_down = jnp.concatenate([left, right], axis=1).reshape(1, 19200)
        return y, mine[0:1], mine[1:2], grad_down

    return jax.shard_map(device_step, mesh=mesh, in_specs=(row_spec, row_spec, flat_spec, flat_spec, flat_spec), out_specs=(row_spec, flat_spec, flat_spec, flat_spec), check_vma=False)
```
